8 devices in a mesh: ey: 4 (over z, y, x), ex: 2 (over core).
Axes of the slice: x: 2, y: 2, z: 1, core: 2. Of those that a mesh axis runs over, the one named last changes fastest.
Arguments:
- x: bfloat16 [1024, 2048], P(('ey', 'ex'))
- kv_k: bfloat16 [1024, 512, 1, 128], P(('ey', 'ex'))
- kv_v: bfloat16 [1024, 512, 1, 128], P(('ey', 'ex'))
- lens: int32 [1024], P(('ey', 'ex'))
- topk_idx: int32 [1024, 6], P(('ey', 'ex'))
- gates: float32 [1024, 6], P(('ey', 'ex'))
- ln1: bfloat16 [2048], replicated
- ln2: bfloat16 [2048], replicated
- wq: bfloat16 [2048, 2048], replicated
- wo: bfloat16 [2048, 2048], replicated
- ws1: bfloat16 [2048, 1408], replicated
- ws3: bfloat16 [2048, 1408], replicated
- ws2: bfloat16 [1408, 2048], replicated
- w1: bfloat16 [64, 2048, 1408], P(('ey', 'ex'))
- w3: bfloat16 [64, 2048, 1408], P(('ey', 'ex'))
- w2: bfloat16 [64, 1408, 2048], P(('ey', 'ex'))
Outputs:
- output: bfloat16 [1024, 2048], P(('ey', 'ex'))
All inputs are finite; a program needn't handle non-finite values.
Results may differ from the reference program's by a relative error of at most 0.0124819.
Values are sent between devices in bfloat16 or wider.
A program may use at most 1 GiB of HBM per device.

```python
import jax
import jax.numpy as jnp
from jax import lax

EY = 4
EX = 2
TOKENS = 128
LEN = 512
D = 2048
HEADS = 16
KV_HEADS = 1
HEAD = 128
FF = 1408
EXPERTS = 64
TOP = 6
ROWS_MAX = 2
CAP = 24
EPS = 1e-6
GATE_SCALE = 2.5

NDEV = EY * EX
NT = NDEV * TOKENS
EROW = EXPERTS // EY
NSLOT = EXPERTS * NDEV * CAP


def _normal(key, shape, scale):
    return (scale * jax.random.normal(key, shape, jnp.float32)).astype(jnp.bfloat16)


def _stack(key, n, shape, scale):
    return lax.map(lambda k: _normal(k, shape, scale), jax.random.split(key, n))


def _route(key):
    place_key, token_key = jax.random.split(key)
    places = jax.random.permutation(place_key, jnp.arange(EXPERTS, dtype=jnp.int32))
    half_count = EXPERTS // 2
    upper_span = EXPERTS - 1 - half_count
    offset = places - half_count
    square = offset * offset
    weight = jnp.where(offset < 0, 100 - (square * 78) // (half_count * half_count), 100 + (square * 350) // (upper_span * upper_span)).astype(jnp.uint32)
    row_of = jnp.arange(EXPERTS) // EROW

    def pick_one(one_key):
        order_key, count_key, noise_key = jax.random.split(one_key, 3)
        row_order = jax.random.permutation(order_key, EY)
        rows_used = jax.random.randint(count_key, (), 1, ROWS_MAX + 1)
        allowed = jnp.zeros((EY,), jnp.int32).at[row_order].set((jnp.arange(EY) < rows_used).astype(jnp.int32))
        noise_bits = jax.random.bits(noise_key, (EXPERTS,), jnp.uint32) >> 10
        waiting = jnp.where(allowed[row_of] > 0, noise_bits * weight, jnp.uint32(0xFFFFFFFF))
        return jnp.argsort(waiting)[:TOP]
    return jax.vmap(pick_one)(jax.random.split(token_key, NT)).astype(jnp.int32)


def setup_inputs(seed: int = 0) -> dict:
    ks = jax.random.split(jax.random.key(seed), 16)
    kd = jax.random.split(jax.random.fold_in(jax.random.key(seed), 7), 3)
    hd = HEADS * HEAD
    full = jax.random.uniform(kd[0], (NT,), jnp.float32) < 0.3
    short = jax.random.randint(kd[1], (NT,), 1, LEN // 8 + 1, jnp.int32)
    return {
        'x': _normal(ks[0], (NT, D), 1.0),
        'kv_k': _stack(ks[1], NT, (LEN, KV_HEADS, HEAD), 2.0),
        'kv_v': _stack(ks[2], NT, (LEN, KV_HEADS, HEAD), 1.0),
        'lens': jnp.where(full, LEN, short).astype(jnp.int32),
        'topk_idx': _route(kd[2]),
        'gates': GATE_SCALE * jax.nn.softmax(0.5 * jax.random.normal(ks[5], (NT, TOP), jnp.float32), axis=-1),
        'ln1': (1.0 + 0.1 * jax.random.normal(ks[6], (D,), jnp.float32)).astype(jnp.bfloat16),
        'ln2': (1.0 + 0.1 * jax.random.normal(ks[7], (D,), jnp.float32)).astype(jnp.bfloat16),
        'wq': _normal(ks[8], (D, hd), D ** -0.5),
        'wo': _normal(ks[9], (hd, D), hd ** -0.5),
        'ws1': _normal(ks[10], (D, FF), D ** -0.5),
        'ws3': _normal(ks[11], (D, FF), D ** -0.5),
        'ws2': _normal(ks[12], (FF, D), FF ** -0.5),
        'w1': _stack(ks[13], EXPERTS, (D, FF), D ** -0.5),
        'w3': _stack(ks[14], EXPERTS, (D, FF), D ** -0.5),
        'w2': _stack(ks[15], EXPERTS, (FF, D), FF ** -0.5),
    }


def _rms(v, w):
    v = v.astype(jnp.float32)
    r = lax.rsqrt(jnp.mean(v * v, axis=-1, keepdims=True) + EPS)
    return (v * r * w.astype(jnp.float32)).astype(jnp.bfloat16)


def _ffn(u, w1, w3, w2):
    g = jnp.dot(u, w1, preferred_element_type=jnp.float32)
    v = jnp.dot(u, w3, preferred_element_type=jnp.float32)
    z = (jax.nn.silu(g) * v).astype(jnp.bfloat16)
    return jnp.dot(z, w2, preferred_element_type=jnp.float32).astype(jnp.bfloat16)


def _attn(x, kk, vv, lens, ln1, wq, wo):
    b = x.shape[0]
    a = _rms(x, ln1)
    q = jnp.dot(a, wq, preferred_element_type=jnp.float32).astype(jnp.bfloat16)
    q = q.reshape(b, KV_HEADS, HEADS // KV_HEADS, HEAD).astype(jnp.float32)
    s = jnp.einsum('bkgd,blkd->bkgl', q, kk.astype(jnp.float32)) * HEAD ** -0.5
    valid = jnp.arange(LEN)[None, :] < lens[:, None]
    s = jnp.where(valid[:, None, None, :], s, -jnp.inf)
    p = jax.nn.softmax(s, axis=-1).astype(jnp.bfloat16).astype(jnp.float32)
    o = jnp.einsum('bkgl,blkd->bkgd', p, vv.astype(jnp.float32)).astype(jnp.bfloat16)
    attn = jnp.dot(o.reshape(b, HEADS * HEAD), wo, preferred_element_type=jnp.float32)
    return (x.astype(jnp.float32) + attn).astype(jnp.bfloat16)


def _slots(topk_idx, gates):
    chosen = (topk_idx[:, :, None] == jnp.arange(EXPERTS)[None, None, :]).any(axis=1).astype(jnp.int32)
    chosen = chosen.reshape(NDEV, TOKENS, EXPERTS)
    before = (jnp.cumsum(chosen, axis=1) - chosen).reshape(NT, EXPERTS)
    rank = jnp.take_along_axis(before, topk_idx, axis=1)
    src = (jnp.arange(NT, dtype=jnp.int32) // TOKENS)[:, None]
    pos = jnp.where(rank < CAP, (topk_idx * NDEV + src) * CAP + rank, NSLOT).reshape(-1)
    tok = jnp.broadcast_to(jnp.arange(NT, dtype=jnp.int32)[:, None], (NT, TOP)).reshape(-1)
    slot_tok = jnp.full((NSLOT,), NT, jnp.int32).at[pos].set(tok, mode='drop')
    slot_gate = jnp.zeros((NSLOT,), jnp.float32).at[pos].set(gates.reshape(-1), mode='drop')
    return slot_tok.reshape(EXPERTS, NDEV * CAP), slot_gate.reshape(EXPERTS, NDEV * CAP)


def reference(x, kv_k, kv_v, lens, topk_idx, gates, ln1, ln2, wq, wo, ws1, ws3, ws2, w1, w3, w2):
    per_dev = lambda a: a.reshape((NDEV, TOKENS) + a.shape[1:])
    h = lax.map(lambda t: _attn(t[0], t[1], t[2], t[3], ln1, wq, wo),
                (per_dev(x), per_dev(kv_k), per_dev(kv_v), per_dev(lens))).reshape(NT, D)
    u = _rms(h, ln2)
    slot_tok, slot_gate = _slots(topk_idx, gates)
    u_pad = jnp.concatenate([u, jnp.zeros((1, D), jnp.bfloat16)], axis=0)

    def expert(acc, xs):
        tok, gate, a1, a3, a2 = xs
        e = _ffn(u_pad[tok], a1, a3, a2)
        return acc.at[tok].add(gate[:, None] * e.astype(jnp.float32)), None

    routed, _ = lax.scan(expert, jnp.zeros((NT + 1, D), jnp.float32), (slot_tok, slot_gate, w1, w3, w2))
    y = h.astype(jnp.float32) + _ffn(u, ws1, ws3, ws2).astype(jnp.float32) + routed[:NT]
    return y.astype(jnp.bfloat16)
```

```python
import functools

import jax
import jax.numpy as jnp
from jax import lax
from jax.experimental import pallas as pl
from jax.experimental.pallas import tpu as pltpu
from jax.sharding import PartitionSpec as P

EPS = 1e-6
BF = jnp.bfloat16
F32 = jnp.float32
MESH = pl.DeviceIdType.MESH
NK = 4
N1 = 4
N2 = 6
PIECES = 3


def _rms(v, w):
    v = v.astype(F32)
    r = lax.rsqrt(jnp.mean(v * v, axis=-1, keepdims=True) + EPS)
    return (v * r * w.astype(F32)).astype(BF)


def _attn(x, kk, vv, lens, ln1, wq, wo):
    b, l, kvh, dh = kk.shape
    hq = wq.shape[1] // dh
    a = _rms(x, ln1)
    q = jnp.dot(a, wq, preferred_element_type=F32).astype(BF).reshape(b, kvh, hq // kvh, dh)
    s = jnp.einsum('bkgd,blkd->bkgl', q, kk, preferred_element_type=F32) * dh ** -0.5
    valid = jnp.arange(l)[None, :] < lens[:, None]
    s = jnp.where(valid[:, None, None, :], s, -jnp.inf)
    p = jax.nn.softmax(s, axis=-1).astype(BF)
    o = jnp.einsum('bkgl,blkd->bkgd', p, vv, preferred_element_type=F32).astype(BF)
    attn = jnp.dot(o.reshape(b, hq * dh), wo, preferred_element_type=F32)
    return (x.astype(F32) + attn).astype(BF)


def _tables(topk, gates, n_exp, ndev, cap, ex_idx):
    b = topk.shape[0]
    hit = topk.T[None, :, :] == jnp.arange(n_exp, dtype=topk.dtype)[:, None, None]
    chosen = hit.any(axis=1)
    gate = jnp.where(hit, gates.T[None, :, :], 0.0).sum(axis=1)
    tri = (jnp.arange(b)[:, None] < jnp.arange(b)[None, :]).astype(BF)
    before = jnp.dot(chosen.astype(BF), tri, preferred_element_type=F32)
    slot = jnp.where(chosen & (before < cap), before + (cap * ex_idx).astype(F32), -1.0)
    return jnp.stack([slot.reshape(ndev, -1, b), gate.reshape(ndev, -1, b)], axis=1)


def _moe_kernel(dims, u_ref, h_ref, tab_ref, w1, w3, w2, ws1, ws3, ws2, y_ref,
                uall, tabs, sel, wgt, xin, acc, z, zs, sh, outb, d2d, rx1, rx2, r13, r2,
                s13, sw2, tsend, trecv, usend, urecv, uloc, dsend, drecv, psend, precv, qsend, qrecv):
    b, d, ff, el, cap = dims
    cw = d // NK
    pair = 2 * cap
    rows = 4 * pair
    ey = lax.axis_index('ey')
    ex = lax.axis_index('ex')
    me = ey * 2 + ex
    ox = 1 - ex
    cx, cy = ey % 2, ey // 2
    xn = cy * 2 + (1 - cx)
    yn = (1 - cy) * 2 + cx
    dg = (1 - cy) * 2 + (1 - cx)
    partner, xdev, ydev = (ey, ox), (xn, ex), (yn, ex)

    n13 = NK + NK * el
    n2 = NK * (el + 1)

    def cp13(src, slot, i):
        return pltpu.make_async_copy(src, r13.at[slot, i], s13.at[slot, i])

    def start13(s):
        slot = s % N1

        @pl.when(s < NK)
        def _():
            ks = pl.ds(pl.multiple_of(s * cw, cw), cw)
            cp13(ws1.at[ks, :], slot, 0).start()
            cp13(ws3.at[ks, :], slot, 1).start()

        @pl.when(s >= NK)
        def _():
            t = s - NK
            e = t % el
            ks = pl.ds(pl.multiple_of((t // el) * cw, cw), cw)
            cp13(w1.at[e, ks, :], slot, 0).start()
            cp13(w3.at[e, ks, :], slot, 1).start()

    def wait13(s):
        slot = s % N1
        for i in range(2):
            cp13(w1.at[0, pl.ds(0, cw), :], slot, i).wait()

    def start2(j):
        slot = j % N2
        c = j // (el + 1)
        i = j % (el + 1)
        cs = pl.ds(pl.multiple_of(c * cw, cw), cw)

        @pl.when(i < el)
        def _():
            pltpu.make_async_copy(w2.at[i, :, cs], r2.at[slot], sw2.at[slot]).start()

        @pl.when(i == el)
        def _():
            pltpu.make_async_copy(ws2.at[:, cs], r2.at[slot], sw2.at[slot]).start()

    def wait2(j):
        slot = j % N2
        pltpu.make_async_copy(w2.at[0, :, pl.ds(0, cw)], r2.at[slot], sw2.at[slot]).wait()

    for s in range(N1):
        start13(jnp.int32(s))

    barrier = pltpu.get_barrier_semaphore()
    for o in range(1, 8):
        peer = (me + o) % 8
        pl.semaphore_signal(barrier, inc=1, device_id=(peer // 2, peer % 2), device_id_type=MESH)
    pl.semaphore_wait(barrier, 7)

    def ublk(k, chip, e):
        return uall.at[k, chip, pl.ds(pl.multiple_of(e * b, b), b), :]

    def ucopy(k, i, src, chip, e, role, dev):
        return pltpu.make_async_remote_copy(
            src_ref=src, dst_ref=ublk(k, chip, e), send_sem=usend.at[k, i], recv_sem=urecv.at[k, role],
            device_id=dev, device_id_type=MESH)

    def uown(k):
        return u_ref.at[:, pl.ds(k * cw, cw)]

    def direct(k):
        cps = [ucopy(k, 1, uown(k), ey, ex, 1, xdev), ucopy(k, 2, uown(k), ey, ex, 2, ydev),
               ucopy(k, 0, uown(k), ey, ex, 0, partner)]
        for cp in cps:
            cp.start()
        pltpu.make_async_copy(uown(k), ublk(k, ey, ex), uloc.at[k]).start()

    def urcv(k, role, chip, e):
        return ucopy(k, 0, uown(k), chip, e, role, partner)

    def forward(k):
        urcv(k, 1, xn, ex).wait_recv()
        if k % 2 == 0:
            ucopy(k, 3, ublk(k, xn, ex), xn, ex, 3, ydev).start()
        ucopy(k, 4, ublk(k, xn, ex), xn, ex, 4, partner).start()
        urcv(k, 2, yn, ex).wait_recv()
        if k % 2 == 1:
            ucopy(k, 3, ublk(k, yn, ex), yn, ex, 3, xdev).start()
        ucopy(k, 5, ublk(k, yn, ex), yn, ex, 5, partner).start()

    def forward_diag(k):
        urcv(k, 3, dg, ex).wait_recv()
        ucopy(k, 6, ublk(k, dg, ex), dg, ex, 6, partner).start()

    def arrived(k):
        pltpu.make_async_copy(uown(k), ublk(k, ey, ex), uloc.at[k]).wait()
        urcv(k, 0, ey, ox).wait_recv()
        urcv(k, 4, xn, ox).wait_recv()
        urcv(k, 5, yn, ox).wait_recv()
        urcv(k, 6, dg, ox).wait_recv()

    direct(0)

    def tcopy(o, peer):
        return pltpu.make_async_remote_copy(
            src_ref=tab_ref.at[peer], dst_ref=tabs.at[me], send_sem=tsend.at[o - 1], recv_sem=trecv.at[o - 1],
            device_id=(peer // 2, peer % 2), device_id_type=MESH)

    for o in range(1, 8):
        tcopy(o, (me + o) % 8).start()
    tabs[me] = tab_ref[me]
    direct(1)

    def silu_mul(g, v):
        return (g * (1.0 / (1.0 + jnp.exp(-g))) * v).astype(BF)

    nts = [(n, min(512, ff - n)) for n in range(0, ff, 512)]

    for s in range(NK):
        wait13(s)
        for n, nw in nts:
            for i in range(2):
                p = jnp.dot(u_ref[:, s * cw:(s + 1) * cw], r13[s % N1, i, :, n:n + nw], preferred_element_type=F32)
                if s > 0:
                    p = acc[i, 0:b, n:n + nw] + p
                acc[i, 0:b, n:n + nw] = p
        start13(jnp.int32(s + N1))
    for n, nw in nts:
        zs[:, n:n + nw] = silu_mul(acc[0, 0:b, n:n + nw], acc[1, 0:b, n:n + nw])

    for o in range(1, 8):
        src = (me + 8 - o) % 8
        pltpu.make_async_remote_copy(
            src_ref=tab_ref.at[src], dst_ref=tabs.at[src], send_sem=tsend.at[o - 1], recv_sem=trecv.at[o - 1],
            device_id=(src // 2, src % 2), device_id_type=MESH).wait_recv()
    iota = lax.broadcasted_iota(jnp.int32, (pair, 2 * b), 0).astype(F32)

    def build(c, _):
        t = jnp.concatenate([tabs[2 * c, 0], tabs[2 * c + 1, 0]], axis=1)
        g = jnp.concatenate([tabs[2 * c, 1], tabs[2 * c + 1, 1]], axis=1)
        one = []
        gat = []
        for e in range(el):
            m = iota == t[e:e + 1, :]
            one.append(jnp.where(m, 1.0, 0.0))
            gat.append(jnp.where(m, g[e:e + 1, :], 0.0))
        sel[c] = jnp.concatenate(one, axis=0).astype(BF)
        gt = jnp.concatenate(gat, axis=0).T
        for i in range(PIECES):
            piece = gt.astype(BF)
            wgt[i, c] = piece
            gt = gt - piece.astype(F32)
        return 0

    lax.fori_loop(0, 4, build, 0)

    forward(0)
    direct(2)
    forward_diag(0)

    for k in range(NK):
        arrived(k)

        def pick(c, _, k=k):
            r = jnp.dot(sel[c], uall[k, c], preferred_element_type=F32).astype(BF)
            for e in range(el):
                xin[e, pl.ds(pl.multiple_of(c * pair, pair), pair), :] = r[e * pair:(e + 1) * pair, :]
            return 0

        lax.fori_loop(0, 4, pick, 0)

        def zstep(e, _, k=k):
            s = NK + k * el + e
            wait13(s)
            slot = s % N1
            er = pl.ds(pl.multiple_of(e * rows, rows), rows)
            for n, nw in nts:
                ps = []
                for i in range(2):
                    p = jnp.dot(xin[e], r13[slot, i, :, n:n + nw], preferred_element_type=F32)
                    if k > 0:
                        p = acc[i, er, n:n + nw] + p
                    ps.append(p)
                if k < NK - 1:
                    acc[0, er, n:n + nw] = ps[0]
                    acc[1, er, n:n + nw] = ps[1]
                else:
                    z[e, :, n:n + nw] = silu_mul(ps[0], ps[1])
            nxt = s + N1

            @pl.when(nxt < n13)
            def _():
                start13(nxt)

            if k == NK - 1:
                @pl.when(nxt >= n13)
                def _():
                    start2(nxt - n13)
            return 0

        half = el // 2
        lax.fori_loop(0, half, zstep, 0)
        if k + 1 < NK:
            forward(k + 1)
            if k + 3 < NK:
                direct(k + 3)
        lax.fori_loop(half, el, zstep, 0)
        if k + 1 < NK:
            forward_diag(k + 1)
    for j in range(N1, N2):
        start2(jnp.int32(j))

    def part(c, e, chip):
        return acc.at[c // 2, pl.ds(pl.multiple_of((e * 4 + chip) * b, b), b), pl.ds((c % 2) * cw, cw)]

    def nbr(c):
        return (xn, xdev, yn, ydev) if c % 2 == 0 else (yn, ydev, xn, xdev)

    def dcopy(c):
        src = acc.at[c // 2, pl.ds(pl.multiple_of(ox * 4 * b, 4 * b), 4 * b), pl.ds((c % 2) * cw, cw)]
        return pltpu.make_async_remote_copy(
            src_ref=src, dst_ref=d2d.at[c], send_sem=dsend.at[c], recv_sem=drecv.at[c],
            device_id=partner, device_id_type=MESH)

    def pcopy(c, i):
        n1, dev1, n2_, dev2 = nbr(c)
        return pltpu.make_async_remote_copy(
            src_ref=part(c, ex, n1 if i == 0 else dg), dst_ref=rx1.at[c, i], send_sem=psend.at[c, i],
            recv_sem=precv.at[c, i], device_id=dev1, device_id_type=MESH)

    def qcopy(c):
        n1, dev1, n2_, dev2 = nbr(c)
        return pltpu.make_async_remote_copy(
            src_ref=part(c, ex, n2_), dst_ref=rx2.at[c], send_sem=qsend.at[c], recv_sem=qrecv.at[c],
            device_id=dev2, device_id_type=MESH)

    def step_a(c):
        def down(e, _):
            j = c * (el + 1) + e
            wait2(j)
            r = jnp.dot(z[e], r2[j % N2], preferred_element_type=F32).astype(BF)
            for q in range(4):
                outb[q, pl.ds(pl.multiple_of(e * pair, pair), pair), :] = r[q * pair:(q + 1) * pair, :]

            @pl.when(j + N2 < n2)
            def _():
                start2(j + N2)
            return 0

        lax.fori_loop(0, el, down, 0)

        def comb(q, _):
            p = jnp.dot(wgt[0, q], outb[q], preferred_element_type=F32)
            for i in range(1, PIECES):
                p = p + jnp.dot(wgt[i, q], outb[q], preferred_element_type=F32)
            part(c, 0, q)[...] = p[0:b]
            part(c, 1, q)[...] = p[b:2 * b]
            return 0

        lax.fori_loop(0, 4, comb, 0)
        dcopy(c).start()
        j = c * (el + 1) + el
        wait2(jnp.int32(j))
        sh[:, c * cw:(c + 1) * cw] = jnp.dot(zs[...], r2[j % N2], preferred_element_type=F32).astype(BF)
        if j + N2 < n2:
            start2(jnp.int32(j + N2))

    def step_b(c):
        dcopy(c).wait_recv()

        def add(q, _):
            part(c, ex, q)[...] = part(c, ex, q)[...] + d2d[c, pl.ds(pl.multiple_of(q * b, b), b), :]
            return 0

        lax.fori_loop(0, 4, add, 0)
        pcopy(c, 1).start()
        pcopy(c, 0).start()

    def step_c(c):
        n1, dev1, n2_, dev2 = nbr(c)
        pcopy(c, 1).wait_recv()
        pcopy(c, 1).wait_send()
        part(c, ex, n2_)[...] = part(c, ex, n2_)[...] + rx1[c, 1]
        qcopy(c).start()

    def step_d(c):
        pcopy(c, 0).wait_recv()
        qcopy(c).wait_recv()
        cs = slice(c * cw, (c + 1) * cw)
        t = part(c, ex, ey)[...] + rx1[c, 0] + rx2[c]
        y_ref[:, cs] = (h_ref[:, cs].astype(F32) + sh[:, cs].astype(F32) + t).astype(BF)

    step_a(0)
    step_a(1)
    step_b(0)
    step_b(1)
    step_a(2)
    step_c(0)
    step_c(1)
    step_a(3)
    step_b(2)
    step_b(3)
    step_d(0)
    step_d(1)
    step_c(2)
    step_c(3)
    step_d(2)
    step_d(3)

    for o in range(1, 8):
        tcopy(o, (me + o) % 8).wait_send()
    for k in range(NK):
        for i in range(7):
            ucopy(k, i, uown(k), ey, ex, 0, partner).wait_send()
    for c in range(NK):
        dcopy(c).wait_send()
        pcopy(c, 0).wait_send()
        qcopy(c).wait_send()


def _moe(u, h, tab, w1, w3, w2, ws1, ws3, ws2, cap):
    b, d = u.shape
    el, _, ff = w1.shape
    ndev, _, _, _ = tab.shape
    cw = d // NK
    pair = 2 * cap
    rows = 4 * pair
    vm = pl.BlockSpec(memory_space=pltpu.VMEM)
    hb = pl.BlockSpec(memory_space=pltpu.HBM)
    dma = pltpu.SemaphoreType.DMA
    return pl.pallas_call(
        functools.partial(_moe_kernel, (b, d, ff, el, cap)),
        out_shape=jax.ShapeDtypeStruct((b, d), BF),
        in_specs=[vm, vm, vm, hb, hb, hb, hb, hb, hb],
        out_specs=vm,
        scratch_shapes=[
            pltpu.VMEM((NK, 4, 2 * b, cw), BF),
            pltpu.VMEM((ndev, 2, el, b), F32),
            pltpu.VMEM((4, el * pair, 2 * b), BF),
            pltpu.VMEM((PIECES, 4, 2 * b, el * pair), BF),
            pltpu.VMEM((el, rows, cw), BF),
            pltpu.VMEM((2, el * rows, ff), F32),
            pltpu.VMEM((el, rows, ff), BF),
            pltpu.VMEM((b, ff), BF),
            pltpu.VMEM((b, d), BF),
            pltpu.VMEM((4, el * pair, cw), BF),
            pltpu.VMEM((NK, 4 * b, cw), F32),
            pltpu.VMEM((NK, 2, b, cw), F32),
            pltpu.VMEM((NK, b, cw), F32),
            pltpu.VMEM((N1, 2, cw, ff), BF),
            pltpu.VMEM((N2, ff, cw), BF),
            dma((N1, 2)), dma((N2,)),
            dma((7,)), dma((7,)),
            dma((NK, 7)), dma((NK, 7)), dma((NK,)),
            dma((NK,)), dma((NK,)),
            dma((NK, 2)), dma((NK, 2)),
            dma((NK,)), dma((NK,)),
        ],
        compiler_params=pltpu.CompilerParams(
            collective_id=0, has_side_effects=True, vmem_limit_bytes=67043328),
        name='moe',
    )(u, h, tab, w1, w3, w2, ws1, ws3, ws2)


def solution(mesh):
    ey, ex = mesh.shape['ey'], mesh.shape['ex']
    ndev = ey * ex
    rows = P(('ey', 'ex'))
    rep = P()

    def local(x, kv_k, kv_v, lens, topk_idx, gates, ln1, ln2, wq, wo, ws1, ws3, ws2, w1, w3, w2):
        b = x.shape[0]
        n_exp = w1.shape[0] * ndev
        cap = max(4, (2 * b * topk_idx.shape[1] + n_exp - 1) // n_exp)
        tab = _tables(topk_idx, gates, n_exp, ndev, cap, lax.axis_index('ex'))
        h = _attn(x, kv_k, kv_v, lens, ln1, wq, wo)
        u = _rms(h, ln2)
        return _moe(u, h, tab, w1, w3, w2, ws1, ws3, ws2, cap)

    return jax.shard_map(
        local, mesh=mesh,
        in_specs=(rows, rows, rows, rows, rows, rows, rep, rep, rep, rep, rep, rep, rep, rows, rows, rows),
        out_specs=rows, check_vma=False)
```

```python
import functools

import jax
import jax.numpy as jnp
from jax import lax
from jax.experimental import pallas as pl
from jax.experimental.pallas import tpu as pltpu
from jax.sharding import PartitionSpec as P

EPS = 1e-6
BF = jnp.bfloat16
F32 = jnp.float32
MESH = pl.DeviceIdType.MESH
NK = 4
N1 = 4
N2 = 6
GS = 8
NS = 3
PC = 128
PIECES = 3


def _rms(v, w):
    v = v.astype(F32)
    r = lax.rsqrt(jnp.mean(v * v, axis=-1, keepdims=True) + EPS)
    return (v * r * w.astype(F32)).astype(BF)


def _attn_kernel(dims, lens_ref, x_ref, kv_k, kv_v, topk_ref, gates_ref, ln1_ref, ln2_ref, wq, wo,
                 h_ref, u_ref, tab_ref, wqb, wob, kb, vb, qs, os, oall, sq, so, sk):
    b, d, l, dh, nq, el, cap = dims
    hd = nq * dh
    qc = hd // 4
    ng = b // GS
    np_ = GS // 2

    def cpq(n):
        return pltpu.make_async_copy(wq.at[:, pl.ds(n * qc, qc)], wqb.at[n], sq.at[n])

    def cpo(n):
        return pltpu.make_async_copy(wo.at[:, pl.ds(n * qc, qc)], wob.at[n], so.at[n])

    for n in range(4):
        cpq(n).start()

    def nch(s):
        return (lens_ref[s] + PC - 1) // PC

    def cpk(src, dst, g, i, c, which):
        slot = g % NS
        ps = pl.ds(pl.multiple_of(c * PC, PC), PC)
        return pltpu.make_async_copy(
            src.at[g * GS + i, ps, :], dst.at[slot, i // 2, ps, pl.ds((i % 2) * dh, dh)], sk.at[slot, which])

    def fetch(g):
        for i in range(GS):
            def one(c, _, i=i):
                cpk(kv_k, kb, g, i, c, 0).start()
                cpk(kv_v, vb, g, i, c, 1).start()
                return 0
            lax.fori_loop(0, nch(g * GS + i), one, 0)

    def fetched(g):
        n = nch(g * GS)
        for i in range(1, GS):
            n = n + nch(g * GS + i)

        def one(c, _):
            cpk(kv_k, kb, g, 0, 0, 0).wait()
            cpk(kv_v, vb, g, 0, 0, 1).wait()
            return 0
        lax.fori_loop(0, n, one, 0)

    def clear(s, _):
        for p in range(np_):
            kb[s, p] = jnp.zeros((l, 2 * dh), BF)
            vb[s, p] = jnp.zeros((l, 2 * dh), BF)
        return 0
    lax.fori_loop(0, NS, clear, 0)
    for g in range(NS):
        fetch(jnp.int32(g))
    for n in range(4):
        cpo(n).start()

    n_exp = tab_ref.shape[0] * el
    eidx = lax.broadcasted_iota(jnp.int32, (n_exp, b), 0)
    hit = eidx < 0
    gate = jnp.zeros((n_exp, b), F32)
    for j in range(topk_ref.shape[0]):
        m = topk_ref[j:j + 1, :] == eidx
        hit = hit | m
        gate = gate + jnp.where(m, gates_ref[j:j + 1, :], 0.0)
    chosen = jnp.where(hit, 1.0, 0.0)
    tri = jnp.where(lax.broadcasted_iota(jnp.int32, (b, b), 0) < lax.broadcasted_iota(jnp.int32, (b, b), 1), 1.0, 0.0)
    before = jnp.dot(chosen.astype(BF), tri.astype(BF), preferred_element_type=F32)
    off = (lax.axis_index('ex') * cap).astype(F32)
    slot_ = jnp.where(hit & (before < cap), before + off, -1.0)
    for e in range(tab_ref.shape[0]):
        tab_ref[e, 0] = slot_[e * el:(e + 1) * el]
        tab_ref[e, 1] = gate[e * el:(e + 1) * el]

    a = _rms(x_ref[...], ln1_ref[...])
    for n in range(4):
        cpq(n).wait()
        qn = jnp.dot(a, wqb[n], preferred_element_type=F32).astype(BF).astype(F32)
        for i in range(qc // dh):
            qs[:, n * (qc // dh) + i, :] = qn[:, i * dh:(i + 1) * dh]

    pos = lax.broadcasted_iota(jnp.int32, (nq, l), 1)
    zero = jnp.zeros((nq, dh), BF)

    def step(g, _):
        fetched(g)
        slot = g % NS
        for p in range(np_):
            s0 = g * GS + 2 * p
            q0 = jnp.concatenate([qs[s0].astype(BF), zero], axis=1)
            q1 = jnp.concatenate([zero, qs[s0 + 1].astype(BF)], axis=1)
            lhs = jnp.concatenate([q0, q1], axis=0)
            s = lax.dot_general(lhs, kb[slot, p], (((1,), (1,)), ((), ())), preferred_element_type=F32) * dh ** -0.5
            valid = jnp.concatenate([pos < lens_ref[s0], pos < lens_ref[s0 + 1]], axis=0)
            s = jnp.where(valid, s, -jnp.inf)
            e = jnp.exp(s - jnp.max(s, axis=-1, keepdims=True))
            pr = (e * (1.0 / jnp.sum(e, axis=-1, keepdims=True))).astype(BF)
            o = jnp.dot(pr, vb[slot, p], preferred_element_type=F32).astype(BF).astype(F32)
            os[s0] = o[0:nq, 0:dh]
            os[s0 + 1] = o[nq:2 * nq, dh:2 * dh]

        @pl.when(g + NS < ng)
        def _():
            fetch(g + NS)
        return 0

    lax.fori_loop(0, ng, step, 0)
    for i in range(nq):
        oall[:, i * dh:(i + 1) * dh] = os[:, i, :].astype(BF)
    for n in range(4):
        cpo(n).wait()
        cs = slice(n * qc, (n + 1) * qc)
        h_ref[:, cs] = (x_ref[:, cs].astype(F32)
                        + jnp.dot(oall[...], wob[n], preferred_element_type=F32)).astype(BF)
    u_ref[...] = _rms(h_ref[...], ln2_ref[...])


def _attention(x, kv_k, kv_v, lens, topk, gates, ln1, ln2, wq, wo, el, ndev, cap):
    b, d = x.shape
    _, l, kvh, dh = kv_k.shape
    hd = wq.shape[1]
    nq = hd // dh
    vm = pl.BlockSpec(memory_space=pltpu.VMEM)
    hb = pl.BlockSpec(memory_space=pltpu.HBM)
    sm = pl.BlockSpec(memory_space=pltpu.SMEM)
    dma = pltpu.SemaphoreType.DMA
    return pl.pallas_call(
        functools.partial(_attn_kernel, (b, d, l, dh, nq, el, cap)),
        out_shape=(jax.ShapeDtypeStruct((b, d), BF), jax.ShapeDtypeStruct((b, d), BF),
                   jax.ShapeDtypeStruct((ndev, 2, el, b), F32)),
        in_specs=[sm, vm, hb, hb, vm, vm, vm, vm, hb, hb],
        out_specs=(vm, vm, vm),
        scratch_shapes=[
            pltpu.VMEM((4, d, hd // 4), BF),
            pltpu.VMEM((4, hd, d // 4), BF),
            pltpu.VMEM((NS, GS // 2, l, 2 * dh), BF),
            pltpu.VMEM((NS, GS // 2, l, 2 * dh), BF),
            pltpu.VMEM((b, nq, dh), F32),
            pltpu.VMEM((b, nq, dh), F32),
            pltpu.VMEM((b, hd), BF),
            dma((4,)), dma((4,)), dma((NS, 2)),
        ],
        compiler_params=pltpu.CompilerParams(vmem_limit_bytes=56 * 1024 * 1024),
        name='attn',
    )(lens, x, kv_k.reshape(b, l, dh), kv_v.reshape(b, l, dh), topk.T, gates.T,
      ln1.reshape(1, d), ln2.reshape(1, d), wq, wo)


def _moe_kernel(dims, u_ref, h_ref, tab_ref, w1, w3, w2, ws1, ws3, ws2, y_ref,
                uall, tabs, sel, wgt, xin, acc, z, zs, sh, outb, d2d, rx1, rx2, r13, r2,
                s13, sw2, tsend, trecv, usend, urecv, uloc, dsend, drecv, psend, precv, qsend, qrecv):
    b, d, ff, el, cap = dims
    cw = d // NK
    pair = 2 * cap
    rows = 4 * pair
    ey = lax.axis_index('ey')
    ex = lax.axis_index('ex')
    me = ey * 2 + ex
    ox = 1 - ex
    cx, cy = ey % 2, ey // 2
    xn = cy * 2 + (1 - cx)
    yn = (1 - cy) * 2 + cx
    dg = (1 - cy) * 2 + (1 - cx)
    partner, xdev, ydev = (ey, ox), (xn, ex), (yn, ex)

    n13 = NK + NK * el
    n2 = NK * (el + 1)

    def cp13(src, slot, i):
        return pltpu.make_async_copy(src, r13.at[slot, i], s13.at[slot, i])

    def start13(s):
        slot = s % N1

        @pl.when(s < NK)
        def _():
            ks = pl.ds(pl.multiple_of(s * cw, cw), cw)
            cp13(ws1.at[ks, :], slot, 0).start()
            cp13(ws3.at[ks, :], slot, 1).start()

        @pl.when(s >= NK)
        def _():
            t = s - NK
            e = t % el
            ks = pl.ds(pl.multiple_of((t // el) * cw, cw), cw)
            cp13(w1.at[e, ks, :], slot, 0).start()
            cp13(w3.at[e, ks, :], slot, 1).start()

    def wait13(s):
        slot = s % N1
        for i in range(2):
            cp13(w1.at[0, pl.ds(0, cw), :], slot, i).wait()

    def start2(j):
        slot = j % N2
        c = j // (el + 1)
        i = j % (el + 1)
        cs = pl.ds(pl.multiple_of(c * cw, cw), cw)

        @pl.when(i < el)
        def _():
            pltpu.make_async_copy(w2.at[i, :, cs], r2.at[slot], sw2.at[slot]).start()

        @pl.when(i == el)
        def _():
            pltpu.make_async_copy(ws2.at[:, cs], r2.at[slot], sw2.at[slot]).start()

    def wait2(j):
        slot = j % N2
        pltpu.make_async_copy(w2.at[0, :, pl.ds(0, cw)], r2.at[slot], sw2.at[slot]).wait()

    for s in range(N1):
        start13(jnp.int32(s))

    barrier = pltpu.get_barrier_semaphore()
    for o in range(1, 8):
        peer = (me + o) % 8
        pl.semaphore_signal(barrier, inc=1, device_id=(peer // 2, peer % 2), device_id_type=MESH)
    pl.semaphore_wait(barrier, 7)

    def ublk(k, chip, e):
        return uall.at[k, chip, pl.ds(pl.multiple_of(e * b, b), b), :]

    def ucopy(k, i, src, chip, e, role, dev):
        return pltpu.make_async_remote_copy(
            src_ref=src, dst_ref=ublk(k, chip, e), send_sem=usend.at[k, i], recv_sem=urecv.at[k, role],
            device_id=dev, device_id_type=MESH)

    def uown(k):
        return u_ref.at[:, pl.ds(k * cw, cw)]

    def direct(k):
        cps = [ucopy(k, 1, uown(k), ey, ex, 1, xdev), ucopy(k, 2, uown(k), ey, ex, 2, ydev),
               ucopy(k, 0, uown(k), ey, ex, 0, partner)]
        for cp in cps:
            cp.start()
        pltpu.make_async_copy(uown(k), ublk(k, ey, ex), uloc.at[k]).start()

    def urcv(k, role, chip, e):
        return ucopy(k, 0, uown(k), chip, e, role, partner)

    def forward(k):
        urcv(k, 1, xn, ex).wait_recv()
        if k % 2 == 0:
            ucopy(k, 3, ublk(k, xn, ex), xn, ex, 3, ydev).start()
        ucopy(k, 4, ublk(k, xn, ex), xn, ex, 4, partner).start()
        urcv(k, 2, yn, ex).wait_recv()
        if k % 2 == 1:
            ucopy(k, 3, ublk(k, yn, ex), yn, ex, 3, xdev).start()
        ucopy(k, 5, ublk(k, yn, ex), yn, ex, 5, partner).start()

    def forward_diag(k):
        urcv(k, 3, dg, ex).wait_recv()
        ucopy(k, 6, ublk(k, dg, ex), dg, ex, 6, partner).start()

    def arrived(k):
        pltpu.make_async_copy(uown(k), ublk(k, ey, ex), uloc.at[k]).wait()
        urcv(k, 0, ey, ox).wait_recv()
        urcv(k, 4, xn, ox).wait_recv()
        urcv(k, 5, yn, ox).wait_recv()
        urcv(k, 6, dg, ox).wait_recv()

    direct(0)

    def tcopy(o, peer):
        return pltpu.make_async_remote_copy(
            src_ref=tab_ref.at[peer], dst_ref=tabs.at[me], send_sem=tsend.at[o - 1], recv_sem=trecv.at[o - 1],
            device_id=(peer // 2, peer % 2), device_id_type=MESH)

    for o in range(1, 8):
        tcopy(o, (me + o) % 8).start()
    tabs[me] = tab_ref[me]
    direct(1)

    def silu_mul(g, v):
        return (g * (1.0 / (1.0 + jnp.exp(-g))) * v).astype(BF)

    nts = [(n, min(512, ff - n)) for n in range(0, ff, 512)]

    for s in range(NK):
        wait13(s)
        for n, nw in nts:
            for i in range(2):
                p = jnp.dot(u_ref[:, s * cw:(s + 1) * cw], r13[s % N1, i, :, n:n + nw], preferred_element_type=F32)
                if s > 0:
                    p = acc[i, 0:b, n:n + nw] + p
                acc[i, 0:b, n:n + nw] = p
        start13(jnp.int32(s + N1))
    for n, nw in nts:
        zs[:, n:n + nw] = silu_mul(acc[0, 0:b, n:n + nw], acc[1, 0:b, n:n + nw])

    for o in range(1, 8):
        src = (me + 8 - o) % 8
        pltpu.make_async_remote_copy(
            src_ref=tab_ref.at[src], dst_ref=tabs.at[src], send_sem=tsend.at[o - 1], recv_sem=trecv.at[o - 1],
            device_id=(src // 2, src % 2), device_id_type=MESH).wait_recv()
    iota = lax.broadcasted_iota(jnp.int32, (pair, 2 * b), 0).astype(F32)

    def build(c, _):
        t = jnp.concatenate([tabs[2 * c, 0], tabs[2 * c + 1, 0]], axis=1)
        g = jnp.concatenate([tabs[2 * c, 1], tabs[2 * c + 1, 1]], axis=1)
        one = []
        gat = []
        for e in range(el):
            m = iota == t[e:e + 1, :]
            one.append(jnp.where(m, 1.0, 0.0))
            gat.append(jnp.where(m, g[e:e + 1, :], 0.0))
        sel[c] = jnp.concatenate(one, axis=0).astype(BF)
        gt = jnp.concatenate(gat, axis=0).T
        for i in range(PIECES):
            piece = gt.astype(BF)
            wgt[i, c] = piece
            gt = gt - piece.astype(F32)
        return 0

    lax.fori_loop(0, 4, build, 0)

    forward(0)
    direct(2)
    forward_diag(0)

    for k in range(NK):
        arrived(k)

        def pick(c, _, k=k):
            r = jnp.dot(sel[c], uall[k, c], preferred_element_type=F32).astype(BF)
            for e in range(el):
                xin[e, pl.ds(pl.multiple_of(c * pair, pair), pair), :] = r[e * pair:(e + 1) * pair, :]
            return 0

        lax.fori_loop(0, 4, pick, 0)

        def zstep(e, _, k=k):
            s = NK + k * el + e
            wait13(s)
            slot = s % N1
            er = pl.ds(pl.multiple_of(e * rows, rows), rows)
            for n, nw in nts:
                ps = []
                for i in range(2):
                    p = jnp.dot(xin[e], r13[slot, i, :, n:n + nw], preferred_element_type=F32)
                    if k > 0:
                        p = acc[i, er, n:n + nw] + p
                    ps.append(p)
                if k < NK - 1:
                    acc[0, er, n:n + nw] = ps[0]
                    acc[1, er, n:n + nw] = ps[1]
                else:
                    z[e, :, n:n + nw] = silu_mul(ps[0], ps[1])
            nxt = s + N1

            @pl.when(nxt < n13)
            def _():
                start13(nxt)

            if k == NK - 1:
                @pl.when(nxt >= n13)
                def _():
                    start2(nxt - n13)
            return 0

        half = el // 2
        lax.fori_loop(0, half, zstep, 0)
        if k + 1 < NK:
            forward(k + 1)
            if k + 3 < NK:
                direct(k + 3)
        lax.fori_loop(half, el, zstep, 0)
        if k + 1 < NK:
            forward_diag(k + 1)
    for j in range(N1, N2):
        start2(jnp.int32(j))

    def part(c, e, chip):
        return acc.at[c // 2, pl.ds(pl.multiple_of((e * 4 + chip) * b, b), b), pl.ds((c % 2) * cw, cw)]

    def nbr(c):
        return (xn, xdev, yn, ydev) if c % 2 == 0 else (yn, ydev, xn, xdev)

    def dcopy(c):
        src = acc.at[c // 2, pl.ds(pl.multiple_of(ox * 4 * b, 4 * b), 4 * b), pl.ds((c % 2) * cw, cw)]
        return pltpu.make_async_remote_copy(
            src_ref=src, dst_ref=d2d.at[c], send_sem=dsend.at[c], recv_sem=drecv.at[c],
            device_id=partner, device_id_type=MESH)

    def pcopy(c, i):
        n1, dev1, n2_, dev2 = nbr(c)
        return pltpu.make_async_remote_copy(
            src_ref=part(c, ex, n1 if i == 0 else dg), dst_ref=rx1.at[c, i], send_sem=psend.at[c, i],
            recv_sem=precv.at[c, i], device_id=dev1, device_id_type=MESH)

    def qcopy(c):
        n1, dev1, n2_, dev2 = nbr(c)
        return pltpu.make_async_remote_copy(
            src_ref=part(c, ex, n2_), dst_ref=rx2.at[c], send_sem=qsend.at[c], recv_sem=qrecv.at[c],
            device_id=dev2, device_id_type=MESH)

    def step_a(c):
        def down(e, _):
            j = c * (el + 1) + e
            wait2(j)
            r = jnp.dot(z[e], r2[j % N2], preferred_element_type=F32).astype(BF)
            for q in range(4):
                outb[q, pl.ds(pl.multiple_of(e * pair, pair), pair), :] = r[q * pair:(q + 1) * pair, :]

            @pl.when(j + N2 < n2)
            def _():
                start2(j + N2)
            return 0

        lax.fori_loop(0, el, down, 0)

        def comb(q, _):
            p = jnp.dot(wgt[0, q], outb[q], preferred_element_type=F32)
            for i in range(1, PIECES):
                p = p + jnp.dot(wgt[i, q], outb[q], preferred_element_type=F32)
            part(c, 0, q)[...] = p[0:b]
            part(c, 1, q)[...] = p[b:2 * b]
            return 0

        lax.fori_loop(0, 4, comb, 0)
        dcopy(c).start()
        j = c * (el + 1) + el
        wait2(jnp.int32(j))
        sh[:, c * cw:(c + 1) * cw] = jnp.dot(zs[...], r2[j % N2], preferred_element_type=F32).astype(BF)
        if j + N2 < n2:
            start2(jnp.int32(j + N2))

    def step_b(c):
        dcopy(c).wait_recv()

        def add(q, _):
            part(c, ex, q)[...] = part(c, ex, q)[...] + d2d[c, pl.ds(pl.multiple_of(q * b, b), b), :]
            return 0

        lax.fori_loop(0, 4, add, 0)
        pcopy(c, 1).start()
        pcopy(c, 0).start()

    def step_c(c):
        n1, dev1, n2_, dev2 = nbr(c)
        pcopy(c, 1).wait_recv()
        pcopy(c, 1).wait_send()
        part(c, ex, n2_)[...] = part(c, ex, n2_)[...] + rx1[c, 1]
        qcopy(c).start()

    def step_d(c):
        pcopy(c, 0).wait_recv()
        qcopy(c).wait_recv()
        cs = slice(c * cw, (c + 1) * cw)
        t = part(c, ex, ey)[...] + rx1[c, 0] + rx2[c]
        y_ref[:, cs] = (h_ref[:, cs].astype(F32) + sh[:, cs].astype(F32) + t).astype(BF)

    step_a(0)
    step_a(1)
    step_b(0)
    step_b(1)
    step_a(2)
    step_c(0)
    step_c(1)
    step_a(3)
    step_b(2)
    step_b(3)
    step_d(0)
    step_d(1)
    step_c(2)
    step_c(3)
    step_d(2)
    step_d(3)

    for o in range(1, 8):
        tcopy(o, (me + o) % 8).wait_send()
    for k in range(NK):
        for i in range(7):
            ucopy(k, i, uown(k), ey, ex, 0, partner).wait_send()
    for c in range(NK):
        dcopy(c).wait_send()
        pcopy(c, 0).wait_send()
        qcopy(c).wait_send()


def _moe(u, h, tab, w1, w3, w2, ws1, ws3, ws2, cap):
    b, d = u.shape
    el, _, ff = w1.shape
    ndev, _, _, _ = tab.shape
    cw = d // NK
    pair = 2 * cap
    rows = 4 * pair
    vm = pl.BlockSpec(memory_space=pltpu.VMEM)
    hb = pl.BlockSpec(memory_space=pltpu.HBM)
    dma = pltpu.SemaphoreType.DMA
    return pl.pallas_call(
        functools.partial(_moe_kernel, (b, d, ff, el, cap)),
        out_shape=jax.ShapeDtypeStruct((b, d), BF),
        in_specs=[vm, vm, vm, hb, hb, hb, hb, hb, hb],
        out_specs=vm,
        scratch_shapes=[
            pltpu.VMEM((NK, 4, 2 * b, cw), BF),
            pltpu.VMEM((ndev, 2, el, b), F32),
            pltpu.VMEM((4, el * pair, 2 * b), BF),
            pltpu.VMEM((PIECES, 4, 2 * b, el * pair), BF),
            pltpu.VMEM((el, rows, cw), BF),
            pltpu.VMEM((2, el * rows, ff), F32),
            pltpu.VMEM((el, rows, ff), BF),
            pltpu.VMEM((b, ff), BF),
            pltpu.VMEM((b, d), BF),
            pltpu.VMEM((4, el * pair, cw), BF),
            pltpu.VMEM((NK, 4 * b, cw), F32),
            pltpu.VMEM((NK, 2, b, cw), F32),
            pltpu.VMEM((NK, b, cw), F32),
            pltpu.VMEM((N1, 2, cw, ff), BF),
            pltpu.VMEM((N2, ff, cw), BF),
            dma((N1, 2)), dma((N2,)),
            dma((7,)), dma((7,)),
            dma((NK, 7)), dma((NK, 7)), dma((NK,)),
            dma((NK,)), dma((NK,)),
            dma((NK, 2)), dma((NK, 2)),
            dma((NK,)), dma((NK,)),
        ],
        compiler_params=pltpu.CompilerParams(
            collective_id=0, has_side_effects=True, vmem_limit_bytes=67043328),
        name='moe',
    )(u, h, tab, w1, w3, w2, ws1, ws3, ws2)


def solution(mesh):
    ey, ex = mesh.shape['ey'], mesh.shape['ex']
    ndev = ey * ex
    rows = P(('ey', 'ex'))
    rep = P()

    def local(x, kv_k, kv_v, lens, topk_idx, gates, ln1, ln2, wq, wo, ws1, ws3, ws2, w1, w3, w2):
        b = x.shape[0]
        n_exp = w1.shape[0] * ndev
        cap = max(4, (2 * b * topk_idx.shape[1] + n_exp - 1) // n_exp)
        h, u, tab = _attention(x, kv_k, kv_v, lens, topk_idx, gates, ln1, ln2, wq, wo, w1.shape[0], ndev, cap)
        return _moe(u, h, tab, w1, w3, w2, ws1, ws3, ws2, cap)

    return jax.shard_map(
        local, mesh=mesh,
        in_specs=(rows, rows, rows, rows, rows, rows, rep, rep, rep, rep, rep, rep, rep, rows, rows, rows),
        out_specs=rows, check_vma=False)
```

```python
import functools

import jax
import jax.numpy as jnp
from jax import lax
from jax.experimental import pallas as pl
from jax.experimental.pallas import tpu as pltpu
from jax.sharding import PartitionSpec as P

EPS = 1e-6
BF = jnp.bfloat16
F32 = jnp.float32
MESH = pl.DeviceIdType.MESH
NK = 4
N1 = 4
N2 = 6
GS = 8
NS = 5
SHORT = 64
PIECES = 3


def _rms(v, w):
    v = v.astype(F32)
    r = lax.rsqrt(jnp.mean(v * v, axis=-1, keepdims=True) + EPS)
    return (v * r * w.astype(F32)).astype(BF)


def _attn_kernel(dims, lens_ref, x_ref, kv_k, kv_v, topk_ref, gates_ref, ln1_ref, ln2_ref, wq, wo,
                 h_ref, u_ref, tab_ref, wqb, wob, kb, vb, qs, os, oall, sb, pb, sq, so, sk):
    b, d, l, dh, nq, el, cap = dims
    hd = nq * dh
    qc = hd // 4
    ng = b // GS
    np_ = GS // 2

    def cpq(n):
        return pltpu.make_async_copy(wq.at[:, pl.ds(n * qc, qc)], wqb.at[n], sq.at[n])

    def cpo(n):
        return pltpu.make_async_copy(wo.at[:, pl.ds(n * qc, qc)], wob.at[n], so.at[n])

    for n in range(4):
        cpq(n).start()

    def fetch(g):
        slot = g % NS
        for i in range(GS):
            ls = pl.ds((i % 2) * dh, dh)
            full = lens_ref[g * GS + i] > SHORT
            for cond, n in ((full, l), (jnp.logical_not(full), SHORT)):
                @pl.when(cond)
                def _(i=i, n=n, ls=ls):
                    for src, dst in ((kv_k, kb), (kv_v, vb)):
                        pltpu.make_async_copy(
                            src.at[g * GS + i, pl.ds(0, n), :], dst.at[slot, i // 2, pl.ds(0, n), ls],
                            sk.at[slot]).start()

    def fetched(g):
        slot = g % NS
        for i in range(GS):
            full = lens_ref[g * GS + i] > SHORT
            for cond, n in ((full, l), (jnp.logical_not(full), SHORT)):
                @pl.when(cond)
                def _(n=n):
                    blk = kb.at[slot, 0, pl.ds(0, n), :]
                    pltpu.make_async_copy(blk, blk, sk.at[slot]).wait()

    def clear(s, _):
        for p in range(np_):
            kb[s, p] = jnp.zeros((l, 2 * dh), BF)
            vb[s, p] = jnp.zeros((l, 2 * dh), BF)
        return 0
    lax.fori_loop(0, NS, clear, 0)
    for g in range(NS - 2):
        fetch(jnp.int32(g))
    for n in range(4):
        cpo(n).start()

    n_exp = tab_ref.shape[0] * el
    eidx = lax.broadcasted_iota(jnp.int32, (n_exp, b), 0)
    hit = eidx < 0
    gate = jnp.zeros((n_exp, b), F32)
    for j in range(topk_ref.shape[0]):
        m = topk_ref[j:j + 1, :] == eidx
        hit = hit | m
        gate = gate + jnp.where(m, gates_ref[j:j + 1, :], 0.0)
    chosen = jnp.where(hit, 1.0, 0.0)
    tri = jnp.where(lax.broadcasted_iota(jnp.int32, (b, b), 0) < lax.broadcasted_iota(jnp.int32, (b, b), 1), 1.0, 0.0)
    before = jnp.dot(chosen.astype(BF), tri.astype(BF), preferred_element_type=F32)
    off = (lax.axis_index('ex') * cap).astype(F32)
    slot_ = jnp.where(hit & (before < cap), before + off, -1.0)
    for e in range(tab_ref.shape[0]):
        tab_ref[e, 0] = slot_[e * el:(e + 1) * el]
        tab_ref[e, 1] = gate[e * el:(e + 1) * el]

    a = _rms(x_ref[...], ln1_ref[...].reshape(1, d))
    for n in range(4):
        cpq(n).wait()
        qn = jnp.dot(a, wqb[n], preferred_element_type=F32).astype(BF).astype(F32)
        for i in range(qc // dh):
            qs[:, n * (qc // dh) + i, :] = qn[:, i * dh:(i + 1) * dh]

    pos = lax.broadcasted_iota(jnp.int32, (nq, l), 1)
    zero = jnp.zeros((nq, dh), BF)

    def scores(g):
        slot = g % NS
        for p in range(np_):
            s0 = g * GS + 2 * p
            q0 = jnp.concatenate([qs[s0].astype(BF), zero], axis=1)
            q1 = jnp.concatenate([zero, qs[s0 + 1].astype(BF)], axis=1)
            lhs = jnp.concatenate([q0, q1], axis=0)
            sb[p] = lax.dot_general(lhs, kb[slot, p], (((1,), (1,)), ((), ())), preferred_element_type=F32)

    def softmax(g):
        for p in range(np_):
            s0 = g * GS + 2 * p
            valid = jnp.concatenate([pos < lens_ref[s0], pos < lens_ref[s0 + 1]], axis=0)
            s = jnp.where(valid, sb[p] * dh ** -0.5, -jnp.inf)
            e = jnp.exp(s - jnp.max(s, axis=-1, keepdims=True))
            pb[p] = (e * (1.0 / jnp.sum(e, axis=-1, keepdims=True))).astype(BF)

    def values(g):
        slot = g % NS
        for p in range(np_):
            s0 = g * GS + 2 * p
            o = jnp.dot(pb[p], vb[slot, p], preferred_element_type=F32).astype(BF).astype(F32)
            os[s0] = o[0:nq, 0:dh]
            os[s0 + 1] = o[nq:2 * nq, dh:2 * dh]

    fetched(jnp.int32(0))
    scores(jnp.int32(0))
    fetch(jnp.int32(NS - 2))
    fetched(jnp.int32(1))
    softmax(jnp.int32(0))
    scores(jnp.int32(1))
    fetch(jnp.int32(NS - 1))

    def step(g, _):
        fetched(g)
        values(g - 2)
        softmax(g - 1)
        scores(g)

        @pl.when(g - 2 + NS < ng)
        def _():
            fetch(g - 2 + NS)
        return 0

    lax.fori_loop(2, ng, step, 0)
    values(jnp.int32(ng - 2))
    softmax(jnp.int32(ng - 1))
    values(jnp.int32(ng - 1))
    for i in range(nq):
        oall[:, i * dh:(i + 1) * dh] = os[:, i, :].astype(BF)
    for n in range(4):
        cpo(n).wait()
        cs = slice(n * qc, (n + 1) * qc)
        h_ref[:, cs] = (x_ref[:, cs].astype(F32)
                        + jnp.dot(oall[...], wob[n], preferred_element_type=F32)).astype(BF)
    u_ref[...] = _rms(h_ref[...], ln2_ref[...].reshape(1, d))


def _attention(x, kv_k, kv_v, lens, topk, gates, ln1, ln2, wq, wo, el, ndev, cap):
    b, d = x.shape
    _, l, kvh, dh = kv_k.shape
    hd = wq.shape[1]
    nq = hd // dh
    vm = pl.BlockSpec(memory_space=pltpu.VMEM)
    hb = pl.BlockSpec(memory_space=pltpu.HBM)
    sm = pl.BlockSpec(memory_space=pltpu.SMEM)
    dma = pltpu.SemaphoreType.DMA
    return pl.pallas_call(
        functools.partial(_attn_kernel, (b, d, l, dh, nq, el, cap)),
        out_shape=(jax.ShapeDtypeStruct((b, d), BF), jax.ShapeDtypeStruct((b, d), BF),
                   jax.ShapeDtypeStruct((ndev, 2, el, b), F32)),
        in_specs=[sm, vm, hb, hb, vm, vm, vm, vm, hb, hb],
        out_specs=(vm, vm, vm),
        scratch_shapes=[
            pltpu.VMEM((4, d, hd // 4), BF),
            pltpu.VMEM((4, hd, d // 4), BF),
            pltpu.VMEM((NS, GS // 2, l, 2 * dh), BF),
            pltpu.VMEM((NS, GS // 2, l, 2 * dh), BF),
            pltpu.VMEM((b, nq, dh), F32),
            pltpu.VMEM((b, nq, dh), F32),
            pltpu.VMEM((b, hd), BF),
            pltpu.VMEM((GS // 2, 2 * nq, l), F32),
            pltpu.VMEM((GS // 2, 2 * nq, l), BF),
            dma((4,)), dma((4,)), dma((NS,)),
        ],
        compiler_params=pltpu.CompilerParams(vmem_limit_bytes=56 * 1024 * 1024),
        name='attn',
    )(lens, x, kv_k.reshape(b, l, dh), kv_v.reshape(b, l, dh), topk.T, gates.T,
      ln1, ln2, wq, wo)


def _moe_kernel(dims, u_ref, h_ref, tab_ref, w1, w3, w2, ws1, ws3, ws2, y_ref,
                uall, tabs, sel, wgt, xin, acc, z, zs, sh, outb, d2d, rx1, rx2, r13, r2,
                s13, sw2, tsend, trecv, usend, urecv, uloc, dsend, drecv, psend, precv, qsend, qrecv):
    b, d, ff, el, cap = dims
    cw = d // NK
    pair = 2 * cap
    rows = 4 * pair
    ey = lax.axis_index('ey')
    ex = lax.axis_index('ex')
    me = ey * 2 + ex
    ox = 1 - ex
    cx, cy = ey % 2, ey // 2
    xn = cy * 2 + (1 - cx)
    yn = (1 - cy) * 2 + cx
    dg = (1 - cy) * 2 + (1 - cx)
    partner, xdev, ydev = (ey, ox), (xn, ex), (yn, ex)

    n13 = NK + NK * el
    n2 = NK * (el + 1)

    def cp13(src, slot, i):
        return pltpu.make_async_copy(src, r13.at[slot, i], s13.at[slot, i])

    def start13(s):
        slot = s % N1

        @pl.when(s < NK)
        def _():
            ks = pl.ds(pl.multiple_of(s * cw, cw), cw)
            cp13(ws1.at[ks, :], slot, 0).start()
            cp13(ws3.at[ks, :], slot, 1).start()

        @pl.when(s >= NK)
        def _():
            t = s - NK
            e = t % el
            ks = pl.ds(pl.multiple_of((t // el) * cw, cw), cw)
            cp13(w1.at[e, ks, :], slot, 0).start()
            cp13(w3.at[e, ks, :], slot, 1).start()

    def wait13(s):
        slot = s % N1
        for i in range(2):
            cp13(w1.at[0, pl.ds(0, cw), :], slot, i).wait()

    def start2(j):
        slot = j % N2
        c = j // (el + 1)
        i = j % (el + 1)
        cs = pl.ds(pl.multiple_of(c * cw, cw), cw)

        @pl.when(i < el)
        def _():
            pltpu.make_async_copy(w2.at[i, :, cs], r2.at[slot], sw2.at[slot]).start()

        @pl.when(i == el)
        def _():
            pltpu.make_async_copy(ws2.at[:, cs], r2.at[slot], sw2.at[slot]).start()

    def wait2(j):
        slot = j % N2
        pltpu.make_async_copy(w2.at[0, :, pl.ds(0, cw)], r2.at[slot], sw2.at[slot]).wait()

    for s in range(N1):
        start13(jnp.int32(s))

    barrier = pltpu.get_barrier_semaphore()
    for o in range(1, 8):
        peer = (me + o) % 8
        pl.semaphore_signal(barrier, inc=1, device_id=(peer // 2, peer % 2), device_id_type=MESH)
    pl.semaphore_wait(barrier, 7)

    def ublk(k, chip, e):
        return uall.at[k, chip, pl.ds(pl.multiple_of(e * b, b), b), :]

    def ucopy(k, i, src, chip, e, role, dev):
        return pltpu.make_async_remote_copy(
            src_ref=src, dst_ref=ublk(k, chip, e), send_sem=usend.at[k, i], recv_sem=urecv.at[k, role],
            device_id=dev, device_id_type=MESH)

    def uown(k):
        return u_ref.at[:, pl.ds(k * cw, cw)]

    def direct(k):
        cps = [ucopy(k, 1, uown(k), ey, ex, 1, xdev), ucopy(k, 2, uown(k), ey, ex, 2, ydev),
               ucopy(k, 0, uown(k), ey, ex, 0, partner)]
        for cp in cps:
            cp.start()
        pltpu.make_async_copy(uown(k), ublk(k, ey, ex), uloc.at[k]).start()

    def urcv(k, role, chip, e):
        return ucopy(k, 0, uown(k), chip, e, role, partner)

    def forward(k):
        urcv(k, 1, xn, ex).wait_recv()
        if k % 2 == 0:
            ucopy(k, 3, ublk(k, xn, ex), xn, ex, 3, ydev).start()
        ucopy(k, 4, ublk(k, xn, ex), xn, ex, 4, partner).start()
        urcv(k, 2, yn, ex).wait_recv()
        if k % 2 == 1:
            ucopy(k, 3, ublk(k, yn, ex), yn, ex, 3, xdev).start()
        ucopy(k, 5, ublk(k, yn, ex), yn, ex, 5, partner).start()

    def forward_diag(k):
        urcv(k, 3, dg, ex).wait_recv()
        ucopy(k, 6, ublk(k, dg, ex), dg, ex, 6, partner).start()

    def arrived(k):
        pltpu.make_async_copy(uown(k), ublk(k, ey, ex), uloc.at[k]).wait()
        urcv(k, 0, ey, ox).wait_recv()
        urcv(k, 4, xn, ox).wait_recv()
        urcv(k, 5, yn, ox).wait_recv()
        urcv(k, 6, dg, ox).wait_recv()

    direct(0)

    def tcopy(o, peer):
        return pltpu.make_async_remote_copy(
            src_ref=tab_ref.at[peer], dst_ref=tabs.at[me], send_sem=tsend.at[o - 1], recv_sem=trecv.at[o - 1],
            device_id=(peer // 2, peer % 2), device_id_type=MESH)

    for o in range(1, 8):
        tcopy(o, (me + o) % 8).start()
    tabs[me] = tab_ref[me]
    direct(1)

    def silu_mul(g, v):
        return (g * (1.0 / (1.0 + jnp.exp(-g))) * v).astype(BF)

    nts = [(n, min(512, ff - n)) for n in range(0, ff, 512)]

    for s in range(NK):
        wait13(s)
        for n, nw in nts:
            for i in range(2):
                p = jnp.dot(u_ref[:, s * cw:(s + 1) * cw], r13[s % N1, i, :, n:n + nw], preferred_element_type=F32)
                if s > 0:
                    p = acc[i, 0:b, n:n + nw] + p
                acc[i, 0:b, n:n + nw] = p
        start13(jnp.int32(s + N1))
    for n, nw in nts:
        zs[:, n:n + nw] = silu_mul(acc[0, 0:b, n:n + nw], acc[1, 0:b, n:n + nw])

    for o in range(1, 8):
        src = (me + 8 - o) % 8
        pltpu.make_async_remote_copy(
            src_ref=tab_ref.at[src], dst_ref=tabs.at[src], send_sem=tsend.at[o - 1], recv_sem=trecv.at[o - 1],
            device_id=(src // 2, src % 2), device_id_type=MESH).wait_recv()
    iota = lax.broadcasted_iota(jnp.int32, (pair, 2 * b), 0).astype(F32)

    def build(c, _):
        t = jnp.concatenate([tabs[2 * c, 0], tabs[2 * c + 1, 0]], axis=1)
        g = jnp.concatenate([tabs[2 * c, 1], tabs[2 * c + 1, 1]], axis=1)
        one = []
        gat = []
        for e in range(el):
            m = iota == t[e:e + 1, :]
            one.append(jnp.where(m, 1.0, 0.0))
            gat.append(jnp.where(m, g[e:e + 1, :], 0.0))
        sel[c] = jnp.concatenate(one, axis=0).astype(BF)
        gt = jnp.concatenate(gat, axis=0).T
        for i in range(PIECES):
            piece = gt.astype(BF)
            wgt[i, c] = piece
            gt = gt - piece.astype(F32)
        return 0

    lax.fori_loop(0, 4, build, 0)

    forward(0)
    direct(2)
    forward_diag(0)

    for k in range(NK):
        arrived(k)

        def pick(c, _, k=k):
            r = jnp.dot(sel[c], uall[k, c], preferred_element_type=F32).astype(BF)
            for e in range(el):
                xin[e, pl.ds(pl.multiple_of(c * pair, pair), pair), :] = r[e * pair:(e + 1) * pair, :]
            return 0

        lax.fori_loop(0, 4, pick, 0)

        def zstep(e, _, k=k):
            s = NK + k * el + e
            wait13(s)
            slot = s % N1
            er = pl.ds(pl.multiple_of(e * rows, rows), rows)
            for n, nw in nts:
                ps = []
                for i in range(2):
                    p = jnp.dot(xin[e], r13[slot, i, :, n:n + nw], preferred_element_type=F32)
                    if k > 0:
                        p = acc[i, er, n:n + nw] + p
                    ps.append(p)
                if k < NK - 1:
                    acc[0, er, n:n + nw] = ps[0]
                    acc[1, er, n:n + nw] = ps[1]
                else:
                    z[e, :, n:n + nw] = silu_mul(ps[0], ps[1])
            nxt = s + N1

            @pl.when(nxt < n13)
            def _():
                start13(nxt)

            if k == NK - 1:
                @pl.when(nxt >= n13)
                def _():
                    start2(nxt - n13)
            return 0

        half = el // 2
        lax.fori_loop(0, half, zstep, 0)
        if k + 1 < NK:
            forward(k + 1)
            if k + 3 < NK:
                direct(k + 3)
        lax.fori_loop(half, el, zstep, 0)
        if k + 1 < NK:
            forward_diag(k + 1)
    for j in range(N1, N2):
        start2(jnp.int32(j))

    def part(c, e, chip):
        return acc.at[c // 2, pl.ds(pl.multiple_of((e * 4 + chip) * b, b), b), pl.ds((c % 2) * cw, cw)]

    def nbr(c):
        return (xn, xdev, yn, ydev) if c % 2 == 0 else (yn, ydev, xn, xdev)

    def dcopy(c):
        src = acc.at[c // 2, pl.ds(pl.multiple_of(ox * 4 * b, 4 * b), 4 * b), pl.ds((c % 2) * cw, cw)]
        return pltpu.make_async_remote_copy(
            src_ref=src, dst_ref=d2d.at[c], send_sem=dsend.at[c], recv_sem=drecv.at[c],
            device_id=partner, device_id_type=MESH)

    def pcopy(c, i):
        n1, dev1, n2_, dev2 = nbr(c)
        return pltpu.make_async_remote_copy(
            src_ref=part(c, ex, n1 if i == 0 else dg), dst_ref=rx1.at[c, i], send_sem=psend.at[c, i],
            recv_sem=precv.at[c, i], device_id=dev1, device_id_type=MESH)

    def qcopy(c):
        n1, dev1, n2_, dev2 = nbr(c)
        return pltpu.make_async_remote_copy(
            src_ref=part(c, ex, n2_), dst_ref=rx2.at[c], send_sem=qsend.at[c], recv_sem=qrecv.at[c],
            device_id=dev2, device_id_type=MESH)

    def step_a(c):
        def down(e, _):
            j = c * (el + 1) + e
            wait2(j)
            r = jnp.dot(z[e], r2[j % N2], preferred_element_type=F32).astype(BF)
            for q in range(4):
                outb[q, pl.ds(pl.multiple_of(e * pair, pair), pair), :] = r[q * pair:(q + 1) * pair, :]

            @pl.when(j + N2 < n2)
            def _():
                start2(j + N2)
            return 0

        lax.fori_loop(0, el, down, 0)

        def comb(q, _):
            p = jnp.dot(wgt[0, q], outb[q], preferred_element_type=F32)
            for i in range(1, PIECES):
                p = p + jnp.dot(wgt[i, q], outb[q], preferred_element_type=F32)
            part(c, 0, q)[...] = p[0:b]
            part(c, 1, q)[...] = p[b:2 * b]
            return 0

        lax.fori_loop(0, 4, comb, 0)
        dcopy(c).start()
        j = c * (el + 1) + el
        wait2(jnp.int32(j))
        sh[:, c * cw:(c + 1) * cw] = jnp.dot(zs[...], r2[j % N2], preferred_element_type=F32).astype(BF)
        if j + N2 < n2:
            start2(jnp.int32(j + N2))

    def step_b(c):
        dcopy(c).wait_recv()

        def add(q, _):
            part(c, ex, q)[...] = part(c, ex, q)[...] + d2d[c, pl.ds(pl.multiple_of(q * b, b), b), :]
            return 0

        lax.fori_loop(0, 4, add, 0)
        pcopy(c, 1).start()
        pcopy(c, 0).start()

    def step_c(c):
        n1, dev1, n2_, dev2 = nbr(c)
        pcopy(c, 1).wait_recv()
        pcopy(c, 1).wait_send()
        part(c, ex, n2_)[...] = part(c, ex, n2_)[...] + rx1[c, 1]
        qcopy(c).start()

    def step_d(c):
        pcopy(c, 0).wait_recv()
        qcopy(c).wait_recv()
        cs = slice(c * cw, (c + 1) * cw)
        t = part(c, ex, ey)[...] + rx1[c, 0] + rx2[c]
        y_ref[:, cs] = (h_ref[:, cs].astype(F32) + sh[:, cs].astype(F32) + t).astype(BF)

    step_a(0)
    step_a(1)
    step_b(0)
    step_b(1)
    step_a(2)
    step_c(0)
    step_c(1)
    step_a(3)
    step_b(2)
    step_b(3)
    step_d(0)
    step_d(1)
    step_c(2)
    step_c(3)
    step_d(2)
    step_d(3)

    for o in range(1, 8):
        tcopy(o, (me + o) % 8).wait_send()
    for k in range(NK):
        for i in range(7):
            ucopy(k, i, uown(k), ey, ex, 0, partner).wait_send()
    for c in range(NK):
        dcopy(c).wait_send()
        pcopy(c, 0).wait_send()
        qcopy(c).wait_send()


def _moe(u, h, tab, w1, w3, w2, ws1, ws3, ws2, cap):
    b, d = u.shape
    el, _, ff = w1.shape
    ndev, _, _, _ = tab.shape
    cw = d // NK
    pair = 2 * cap
    rows = 4 * pair
    vm = pl.BlockSpec(memory_space=pltpu.VMEM)
    hb = pl.BlockSpec(memory_space=pltpu.HBM)
    dma = pltpu.SemaphoreType.DMA
    return pl.pallas_call(
        functools.partial(_moe_kernel, (b, d, ff, el, cap)),
        out_shape=jax.ShapeDtypeStruct((b, d), BF),
        in_specs=[vm, vm, vm, hb, hb, hb, hb, hb, hb],
        out_specs=vm,
        scratch_shapes=[
            pltpu.VMEM((NK, 4, 2 * b, cw), BF),
            pltpu.VMEM((ndev, 2, el, b), F32),
            pltpu.VMEM((4, el * pair, 2 * b), BF),
            pltpu.VMEM((PIECES, 4, 2 * b, el * pair), BF),
            pltpu.VMEM((el, rows, cw), BF),
            pltpu.VMEM((2, el * rows, ff), F32),
            pltpu.VMEM((el, rows, ff), BF),
            pltpu.VMEM((b, ff), BF),
            pltpu.VMEM((b, d), BF),
            pltpu.VMEM((4, el * pair, cw), BF),
            pltpu.VMEM((NK, 4 * b, cw), F32),
            pltpu.VMEM((NK, 2, b, cw), F32),
            pltpu.VMEM((NK, b, cw), F32),
            pltpu.VMEM((N1, 2, cw, ff), BF),
            pltpu.VMEM((N2, ff, cw), BF),
            dma((N1, 2)), dma((N2,)),
            dma((7,)), dma((7,)),
            dma((NK, 7)), dma((NK, 7)), dma((NK,)),
            dma((NK,)), dma((NK,)),
            dma((NK, 2)), dma((NK, 2)),
            dma((NK,)), dma((NK,)),
        ],
        compiler_params=pltpu.CompilerParams(
            collective_id=0, has_side_effects=True, vmem_limit_bytes=67043328),
        name='moe',
    )(u, h, tab, w1, w3, w2, ws1, ws3, ws2)


def solution(mesh):
    ey, ex = mesh.shape['ey'], mesh.shape['ex']
    ndev = ey * ex
    rows = P(('ey', 'ex'))
    rep = P()

    def local(x, kv_k, kv_v, lens, topk_idx, gates, ln1, ln2, wq, wo, ws1, ws3, ws2, w1, w3, w2):
        b = x.shape[0]
        n_exp = w1.shape[0] * ndev
        cap = max(4, (2 * b * topk_idx.shape[1] + n_exp - 1) // n_exp)
        h, u, tab = _attention(x, kv_k, kv_v, lens, topk_idx, gates, ln1, ln2, wq, wo, w1.shape[0], ndev, cap)
        return _moe(u, h, tab, w1, w3, w2, ws1, ws3, ws2, cap)

    return jax.shard_map(
        local, mesh=mesh,
        in_specs=(rows, rows, rows, rows, rows, rows, rep, rep, rep, rep, rep, rep, rep, rows, rows, rows),
        out_specs=rows, check_vma=False)
```

```python
import functools

import jax
import jax.numpy as jnp
from jax import lax
from jax.experimental import pallas as pl
from jax.experimental.pallas import tpu as pltpu
from jax.sharding import PartitionSpec as P

EPS = 1e-6
BF = jnp.bfloat16
F32 = jnp.float32
MESH = pl.DeviceIdType.MESH
NK = 4
N1 = 4
N2 = 6
GS = 8
NS = 5
SHORT = 64
PIECES = 3


def _rms(v, w):
    v = v.astype(F32)
    r = lax.rsqrt(jnp.mean(v * v, axis=-1, keepdims=True) + EPS)
    return (v * r * w.astype(F32)).astype(BF)


def _attn_kernel(dims, lens_ref, x_ref, kv_k, kv_v, topk_ref, gates_ref, ln1_ref, ln2_ref, wq, wo,
                 h_ref, u_ref, tab_ref, wqb, wob, kb, vb, qs, os, oall, sb, pb, sq, so, sk):
    b, d, l, dh, nq, el, cap = dims
    hd = nq * dh
    qc = hd // 4
    ng = b // GS
    np_ = GS // 2

    def cpq(n):
        return pltpu.make_async_copy(wq.at[:, pl.ds(n * qc, qc)], wqb.at[n], sq.at[n])

    def cpo(n):
        return pltpu.make_async_copy(wo.at[:, pl.ds(n * qc, qc)], wob.at[n], so.at[n])

    for n in range(4):
        cpq(n).start()

    def fetch(g):
        slot = g % NS
        for i in range(GS):
            ls = pl.ds((i % 2) * dh, dh)
            full = lens_ref[g * GS + i] > SHORT
            for cond, n in ((full, l), (jnp.logical_not(full), SHORT)):
                @pl.when(cond)
                def _(i=i, n=n, ls=ls):
                    for src, dst in ((kv_k, kb), (kv_v, vb)):
                        pltpu.make_async_copy(
                            src.at[g * GS + i, pl.ds(0, n), :], dst.at[slot, i // 2, pl.ds(0, n), ls],
                            sk.at[slot]).start()

    def fetched(g):
        slot = g % NS
        for i in range(GS):
            full = lens_ref[g * GS + i] > SHORT
            for cond, n in ((full, l), (jnp.logical_not(full), SHORT)):
                @pl.when(cond)
                def _(n=n):
                    blk = kb.at[slot, 0, pl.ds(0, n), :]
                    pltpu.make_async_copy(blk, blk, sk.at[slot]).wait()

    def clear(s, _):
        for p in range(np_):
            kb[s, p] = jnp.zeros((l, 2 * dh), BF)
            vb[s, p] = jnp.zeros((l, 2 * dh), BF)
        return 0
    lax.fori_loop(0, NS, clear, 0)
    for g in range(NS - 2):
        fetch(jnp.int32(g))
    for n in range(4):
        cpo(n).start()

    n_exp = tab_ref.shape[0] * el
    eidx = lax.broadcasted_iota(jnp.int32, (n_exp, b), 0)
    hit = eidx < 0
    gate = jnp.zeros((n_exp, b), F32)
    for j in range(topk_ref.shape[0]):
        m = topk_ref[j:j + 1, :] == eidx
        hit = hit | m
        gate = gate + jnp.where(m, gates_ref[j:j + 1, :], 0.0)
    chosen = jnp.where(hit, 1.0, 0.0)
    tri = jnp.where(lax.broadcasted_iota(jnp.int32, (b, b), 0) < lax.broadcasted_iota(jnp.int32, (b, b), 1), 1.0, 0.0)
    before = jnp.dot(chosen.astype(BF), tri.astype(BF), preferred_element_type=F32)
    off = (lax.axis_index('ex') * cap).astype(F32)
    slot_ = jnp.where(hit & (before < cap), before + off, -1.0)
    for e in range(tab_ref.shape[0]):
        tab_ref[e, 0] = slot_[e * el:(e + 1) * el]
        tab_ref[e, 1] = gate[e * el:(e + 1) * el]

    a = _rms(x_ref[...], ln1_ref[...].reshape(1, d))
    for n in range(4):
        cpq(n).wait()
        qn = jnp.dot(a, wqb[n], preferred_element_type=F32).astype(BF).astype(F32)
        for i in range(qc // dh):
            qs[:, n * (qc // dh) + i, :] = qn[:, i * dh:(i + 1) * dh]

    pos = lax.broadcasted_iota(jnp.int32, (nq, l), 1)
    zero = jnp.zeros((nq, dh), BF)

    def scores(g):
        slot = g % NS
        for p in range(np_):
            s0 = g * GS + 2 * p
            q0 = jnp.concatenate([qs[s0].astype(BF), zero], axis=1)
            q1 = jnp.concatenate([zero, qs[s0 + 1].astype(BF)], axis=1)
            lhs = jnp.concatenate([q0, q1], axis=0)
            sb[p] = lax.dot_general(lhs, kb[slot, p], (((1,), (1,)), ((), ())), preferred_element_type=F32)

    def softmax(g):
        for p in range(np_):
            s0 = g * GS + 2 * p
            valid = jnp.concatenate([pos < lens_ref[s0], pos < lens_ref[s0 + 1]], axis=0)
            s = jnp.where(valid, sb[p] * dh ** -0.5, -jnp.inf)
            e = jnp.exp(s - jnp.max(s, axis=-1, keepdims=True))
            pb[p] = (e * (1.0 / jnp.sum(e, axis=-1, keepdims=True))).astype(BF)

    def values(g):
        slot = g % NS
        for p in range(np_):
            s0 = g * GS + 2 * p
            o = jnp.dot(pb[p], vb[slot, p], preferred_element_type=F32).astype(BF).astype(F32)
            os[s0] = o[0:nq, 0:dh]
            os[s0 + 1] = o[nq:2 * nq, dh:2 * dh]

    fetched(jnp.int32(0))
    scores(jnp.int32(0))
    fetch(jnp.int32(NS - 2))
    fetched(jnp.int32(1))
    softmax(jnp.int32(0))
    scores(jnp.int32(1))
    fetch(jnp.int32(NS - 1))

    def step(g, _):
        fetched(g)
        values(g - 2)
        softmax(g - 1)
        scores(g)

        @pl.when(g - 2 + NS < ng)
        def _():
            fetch(g - 2 + NS)
        return 0

    lax.fori_loop(2, ng, step, 0)
    values(jnp.int32(ng - 2))
    softmax(jnp.int32(ng - 1))
    values(jnp.int32(ng - 1))
    for i in range(nq):
        oall[:, i * dh:(i + 1) * dh] = os[:, i, :].astype(BF)
    for n in range(4):
        cpo(n).wait()
        cs = slice(n * qc, (n + 1) * qc)
        h_ref[:, cs] = (x_ref[:, cs].astype(F32)
                        + jnp.dot(oall[...], wob[n], preferred_element_type=F32)).astype(BF)
    u_ref[...] = _rms(h_ref[...], ln2_ref[...].reshape(1, d))


def _attention(x, kv_k, kv_v, lens, topk, gates, ln1, ln2, wq, wo, el, ndev, cap):
    b, d = x.shape
    _, l, kvh, dh = kv_k.shape
    hd = wq.shape[1]
    nq = hd // dh
    vm = pl.BlockSpec(memory_space=pltpu.VMEM)
    hb = pl.BlockSpec(memory_space=pltpu.HBM)
    sm = pl.BlockSpec(memory_space=pltpu.SMEM)
    dma = pltpu.SemaphoreType.DMA
    return pl.pallas_call(
        functools.partial(_attn_kernel, (b, d, l, dh, nq, el, cap)),
        out_shape=(jax.ShapeDtypeStruct((b, d), BF), jax.ShapeDtypeStruct((b, d), BF),
                   jax.ShapeDtypeStruct((ndev, 2, el, b), F32)),
        in_specs=[sm, vm, hb, hb, vm, vm, vm, vm, hb, hb],
        out_specs=(vm, vm, vm),
        scratch_shapes=[
            pltpu.VMEM((4, d, hd // 4), BF),
            pltpu.VMEM((4, hd, d // 4), BF),
            pltpu.VMEM((NS, GS // 2, l, 2 * dh), BF),
            pltpu.VMEM((NS, GS // 2, l, 2 * dh), BF),
            pltpu.VMEM((b, nq, dh), F32),
            pltpu.VMEM((b, nq, dh), F32),
            pltpu.VMEM((b, hd), BF),
            pltpu.VMEM((GS // 2, 2 * nq, l), F32),
            pltpu.VMEM((GS // 2, 2 * nq, l), BF),
            dma((4,)), dma((4,)), dma((NS,)),
        ],
        compiler_params=pltpu.CompilerParams(vmem_limit_bytes=56 * 1024 * 1024),
        name='attn',
    )(lens, x, kv_k.reshape(b, l, dh), kv_v.reshape(b, l, dh), topk.T, gates.T,
      ln1, ln2, wq, wo)


def _moe_kernel(dims, u_ref, h_ref, tab_ref, w1, w3, w2, ws1, ws3, ws2, y_ref,
                uall, tabs, sel, wgt, xin, acc, z, zs, sh, outb, d2d, rx1, rx2, r13, r2,
                s13, sw2, tsend, trecv, usend, urecv, uloc, dsend, drecv, psend, precv, qsend, qrecv):
    b, d, ff, el, cap = dims
    cw = d // NK
    pair = 2 * cap
    rows = 4 * pair
    ey = lax.axis_index('ey')
    ex = lax.axis_index('ex')
    me = ey * 2 + ex
    ox = 1 - ex
    cx, cy = ey % 2, ey // 2
    xn = cy * 2 + (1 - cx)
    yn = (1 - cy) * 2 + cx
    dg = (1 - cy) * 2 + (1 - cx)
    partner, xdev, ydev = (ey, ox), (xn, ex), (yn, ex)

    n13 = NK + NK * el
    n2 = NK * (el + 1)

    def cp13(src, slot, i):
        return pltpu.make_async_copy(src, r13.at[slot, i], s13.at[slot, i])

    def start13(s):
        slot = s % N1

        @pl.when(s < NK)
        def _():
            ks = pl.ds(pl.multiple_of(s * cw, cw), cw)
            cp13(ws1.at[ks, :], slot, 0).start()
            cp13(ws3.at[ks, :], slot, 1).start()

        @pl.when(s >= NK)
        def _():
            t = s - NK
            e = t % el
            ks = pl.ds(pl.multiple_of((t // el) * cw, cw), cw)
            cp13(w1.at[e, ks, :], slot, 0).start()
            cp13(w3.at[e, ks, :], slot, 1).start()

    def wait13(s):
        slot = s % N1
        for i in range(2):
            cp13(w1.at[0, pl.ds(0, cw), :], slot, i).wait()

    def start2(j):
        slot = j % N2
        c = j // (el + 1)
        i = j % (el + 1)
        cs = pl.ds(pl.multiple_of(c * cw, cw), cw)

        @pl.when(i < el)
        def _():
            pltpu.make_async_copy(w2.at[i, :, cs], r2.at[slot], sw2.at[slot]).start()

        @pl.when(i == el)
        def _():
            pltpu.make_async_copy(ws2.at[:, cs], r2.at[slot], sw2.at[slot]).start()

    def wait2(j):
        slot = j % N2
        pltpu.make_async_copy(w2.at[0, :, pl.ds(0, cw)], r2.at[slot], sw2.at[slot]).wait()

    for s in range(N1):
        start13(jnp.int32(s))

    barrier = pltpu.get_barrier_semaphore()
    for o in range(1, 8):
        peer = (me + o) % 8
        pl.semaphore_signal(barrier, inc=1, device_id=(peer // 2, peer % 2), device_id_type=MESH)
    pl.semaphore_wait(barrier, 7)

    def ublk(k, chip, e):
        return uall.at[k, chip, pl.ds(pl.multiple_of(e * b, b), b), :]

    def ucopy(k, i, src, chip, e, role, dev):
        return pltpu.make_async_remote_copy(
            src_ref=src, dst_ref=ublk(k, chip, e), send_sem=usend.at[k, i], recv_sem=urecv.at[k, role],
            device_id=dev, device_id_type=MESH)

    def uown(k):
        return u_ref.at[:, pl.ds(k * cw, cw)]

    def direct(k):
        cps = [ucopy(k, 1, uown(k), ey, ex, 1, xdev), ucopy(k, 2, uown(k), ey, ex, 2, ydev),
               ucopy(k, 0, uown(k), ey, ex, 0, partner)]
        for cp in cps:
            cp.start()
        pltpu.make_async_copy(uown(k), ublk(k, ey, ex), uloc.at[k]).start()

    def urcv(k, role, chip, e):
        return ucopy(k, 0, uown(k), chip, e, role, partner)

    def forward(k):
        urcv(k, 1, xn, ex).wait_recv()
        if k % 2 == 0:
            ucopy(k, 3, ublk(k, xn, ex), xn, ex, 3, ydev).start()
        ucopy(k, 4, ublk(k, xn, ex), xn, ex, 4, partner).start()
        urcv(k, 2, yn, ex).wait_recv()
        if k % 2 == 1:
            ucopy(k, 3, ublk(k, yn, ex), yn, ex, 3, xdev).start()
        ucopy(k, 5, ublk(k, yn, ex), yn, ex, 5, partner).start()

    def forward_diag(k):
        urcv(k, 3, dg, ex).wait_recv()
        ucopy(k, 6, ublk(k, dg, ex), dg, ex, 6, partner).start()

    def arrived(k):
        pltpu.make_async_copy(uown(k), ublk(k, ey, ex), uloc.at[k]).wait()
        urcv(k, 0, ey, ox).wait_recv()
        urcv(k, 4, xn, ox).wait_recv()
        urcv(k, 5, yn, ox).wait_recv()
        urcv(k, 6, dg, ox).wait_recv()

    direct(0)

    def tcopy(o, peer):
        return pltpu.make_async_remote_copy(
            src_ref=tab_ref.at[peer], dst_ref=tabs.at[me], send_sem=tsend.at[o - 1], recv_sem=trecv.at[o - 1],
            device_id=(peer // 2, peer % 2), device_id_type=MESH)

    for o in range(1, 8):
        tcopy(o, (me + o) % 8).start()
    tabs[me] = tab_ref[me]
    direct(1)

    def silu_mul(g, v):
        return (g * (1.0 / (1.0 + jnp.exp(-g))) * v).astype(BF)

    nts = [(n, min(512, ff - n)) for n in range(0, ff, 512)]

    for s in range(NK):
        wait13(s)
        for n, nw in nts:
            for i in range(2):
                p = jnp.dot(u_ref[:, s * cw:(s + 1) * cw], r13[s % N1, i, :, n:n + nw], preferred_element_type=F32)
                if s > 0:
                    p = acc[i, 0:b, n:n + nw] + p
                acc[i, 0:b, n:n + nw] = p
        start13(jnp.int32(s + N1))
    for n, nw in nts:
        zs[:, n:n + nw] = silu_mul(acc[0, 0:b, n:n + nw], acc[1, 0:b, n:n + nw])

    forward(0)
    direct(2)

    for o in range(1, 8):
        src = (me + 8 - o) % 8
        pltpu.make_async_remote_copy(
            src_ref=tab_ref.at[src], dst_ref=tabs.at[src], send_sem=tsend.at[o - 1], recv_sem=trecv.at[o - 1],
            device_id=(src // 2, src % 2), device_id_type=MESH).wait_recv()
    iota = lax.broadcasted_iota(jnp.int32, (pair, 2 * b), 0).astype(F32)

    def build(c, _):
        t = jnp.concatenate([tabs[2 * c, 0], tabs[2 * c + 1, 0]], axis=1)
        g = jnp.concatenate([tabs[2 * c, 1], tabs[2 * c + 1, 1]], axis=1)
        one = []
        gat = []
        for e in range(el):
            m = iota == t[e:e + 1, :]
            one.append(jnp.where(m, 1.0, 0.0))
            gat.append(jnp.where(m, g[e:e + 1, :], 0.0))
        sel[c] = jnp.concatenate(one, axis=0).astype(BF)
        gt = jnp.concatenate(gat, axis=0).T
        for i in range(PIECES):
            piece = gt.astype(BF)
            wgt[i, c] = piece
            gt = gt - piece.astype(F32)
        return 0

    lax.fori_loop(0, 4, build, 0)

    forward(1)
    direct(3)
    forward_diag(0)
    events = {(0, 2): lambda: forward(2), (0, 4): lambda: forward_diag(1), (0, 6): lambda: forward(3),
              (1, 2): lambda: forward_diag(2), (1, 4): lambda: forward_diag(3)}

    for k in range(NK):
        arrived(k)

        def pick(c, _, k=k):
            r = jnp.dot(sel[c], uall[k, c], preferred_element_type=F32).astype(BF)
            for e in range(el):
                xin[e, pl.ds(pl.multiple_of(c * pair, pair), pair), :] = r[e * pair:(e + 1) * pair, :]
            return 0

        lax.fori_loop(0, 4, pick, 0)

        def zstep(e, _, k=k):
            for (ke, at), event in events.items():
                if ke == k:
                    pl.when(e == at)(event)
            s = NK + k * el + e
            wait13(s)
            slot = s % N1
            er = pl.ds(pl.multiple_of(e * rows, rows), rows)
            for n, nw in nts:
                ps = []
                for i in range(2):
                    p = jnp.dot(xin[e], r13[slot, i, :, n:n + nw], preferred_element_type=F32)
                    if k > 0:
                        p = acc[i, er, n:n + nw] + p
                    ps.append(p)
                if k < NK - 1:
                    acc[0, er, n:n + nw] = ps[0]
                    acc[1, er, n:n + nw] = ps[1]
                else:
                    z[e, :, n:n + nw] = silu_mul(ps[0], ps[1])
            nxt = s + N1

            @pl.when(nxt < n13)
            def _():
                start13(nxt)

            if k == NK - 1:
                @pl.when(nxt >= n13)
                def _():
                    start2(nxt - n13)
            return 0

        lax.fori_loop(0, el, zstep, 0)
    for j in range(N1, N2):
        start2(jnp.int32(j))

    hw = cw // 2

    def part(c, e, chip, j=None):
        cols = pl.ds((c % 2) * cw, cw) if j is None else pl.ds((c % 2) * cw + j * hw, hw)
        return acc.at[c // 2, pl.ds(pl.multiple_of((e * 4 + chip) * b, b), b), cols]

    order = ((xn, xdev, yn, ydev), (yn, ydev, xn, xdev))

    def dcopy(c):
        src = acc.at[c // 2, pl.ds(pl.multiple_of(ox * 4 * b, 4 * b), 4 * b), pl.ds((c % 2) * cw, cw)]
        return pltpu.make_async_remote_copy(
            src_ref=src, dst_ref=d2d.at[c], send_sem=dsend.at[c], recv_sem=drecv.at[c],
            device_id=partner, device_id_type=MESH)

    def pcopy(c, j, i):
        first, dev, _, _ = order[j]
        return pltpu.make_async_remote_copy(
            src_ref=part(c, ex, first if i == 0 else dg, j), dst_ref=rx1.at[c, j, i], send_sem=psend.at[c, j, i],
            recv_sem=precv.at[c, j, i], device_id=dev, device_id_type=MESH)

    def qcopy(c, j):
        _, _, second, dev = order[j]
        return pltpu.make_async_remote_copy(
            src_ref=part(c, ex, second, j), dst_ref=rx2.at[c, j], send_sem=qsend.at[c, j], recv_sem=qrecv.at[c, j],
            device_id=dev, device_id_type=MESH)

    def step_a(c, events):
        def down(t, _):
            for at, event in events:
                pl.when(t == at)(event)
            for i in range(2):
                e = 2 * t + i
                j = c * (el + 1) + e
                wait2(j)
                r = jnp.dot(z[e], r2[j % N2], preferred_element_type=F32).astype(BF)
                for q in range(4):
                    outb[q, pl.ds(pl.multiple_of(e * pair, pair), pair), :] = r[q * pair:(q + 1) * pair, :]
            for i in range(2):
                j = c * (el + 1) + 2 * t + i

                @pl.when(j + N2 < n2)
                def _(j=j):
                    start2(j + N2)
            return 0

        lax.fori_loop(0, el // 2, down, 0)

        def comb(t, _):
            for i in range(2):
                q = 2 * t + i
                p = jnp.dot(wgt[0, q], outb[q], preferred_element_type=F32)
                for n in range(1, PIECES):
                    p = p + jnp.dot(wgt[n, q], outb[q], preferred_element_type=F32)
                part(c, 0, q)[...] = p[0:b]
                part(c, 1, q)[...] = p[b:2 * b]
            return 0

        lax.fori_loop(0, 2, comb, 0)
        dcopy(c).start()
        j = c * (el + 1) + el
        wait2(jnp.int32(j))
        sh[:, c * cw:(c + 1) * cw] = jnp.dot(zs[...], r2[j % N2], preferred_element_type=F32).astype(BF)
        if j + N2 < n2:
            start2(jnp.int32(j + N2))

    def step_b(c):
        dcopy(c).wait_recv()

        def add(q, _):
            part(c, ex, q)[...] = part(c, ex, q)[...] + d2d[c, pl.ds(pl.multiple_of(q * b, b), b), :]
            return 0

        lax.fori_loop(0, 4, add, 0)
        for i in (1, 0):
            for j in range(2):
                pcopy(c, j, i).start()

    def step_c(c):
        for j in range(2):
            pcopy(c, j, 1).wait_recv()
            second = order[j][2]
            part(c, ex, second, j)[...] = part(c, ex, second, j)[...] + rx1[c, j, 1]
            qcopy(c, j).start()

    def step_d(c):
        for j in range(2):
            pcopy(c, j, 0).wait_recv()
            qcopy(c, j).wait_recv()
            cs = slice(c * cw + j * hw, c * cw + (j + 1) * hw)
            t = part(c, ex, ey, j)[...] + rx1[c, j, 0] + rx2[c, j]
            y_ref[:, cs] = (h_ref[:, cs].astype(F32) + sh[:, cs].astype(F32) + t).astype(BF)

    step_a(0, ())
    step_a(1, ((2, lambda: step_b(0)),))
    step_a(2, ((1, lambda: step_c(0)), (2, lambda: step_b(1))))
    step_a(3, ((2, lambda: step_b(2)), (3, lambda: step_c(1))))
    step_b(3)
    step_c(2)
    step_d(0)
    step_d(1)
    step_c(3)
    step_d(2)
    step_d(3)

    for o in range(1, 8):
        tcopy(o, (me + o) % 8).wait_send()
    for k in range(NK):
        for i in range(7):
            ucopy(k, i, uown(k), ey, ex, 0, partner).wait_send()
    for c in range(NK):
        dcopy(c).wait_send()
        for j in range(2):
            pcopy(c, j, 0).wait_send()
            pcopy(c, j, 1).wait_send()
            qcopy(c, j).wait_send()


def _moe(u, h, tab, w1, w3, w2, ws1, ws3, ws2, cap):
    b, d = u.shape
    el, _, ff = w1.shape
    ndev, _, _, _ = tab.shape
    cw = d // NK
    pair = 2 * cap
    rows = 4 * pair
    vm = pl.BlockSpec(memory_space=pltpu.VMEM)
    hb = pl.BlockSpec(memory_space=pltpu.HBM)
    dma = pltpu.SemaphoreType.DMA
    return pl.pallas_call(
        functools.partial(_moe_kernel, (b, d, ff, el, cap)),
        out_shape=jax.ShapeDtypeStruct((b, d), BF),
        in_specs=[vm, vm, vm, hb, hb, hb, hb, hb, hb],
        out_specs=vm,
        scratch_shapes=[
            pltpu.VMEM((NK, 4, 2 * b, cw), BF),
            pltpu.VMEM((ndev, 2, el, b), F32),
            pltpu.VMEM((4, el * pair, 2 * b), BF),
            pltpu.VMEM((PIECES, 4, 2 * b, el * pair), BF),
            pltpu.VMEM((el, rows, cw), BF),
            pltpu.VMEM((2, el * rows, ff), F32),
            pltpu.VMEM((el, rows, ff), BF),
            pltpu.VMEM((b, ff), BF),
            pltpu.VMEM((b, d), BF),
            pltpu.VMEM((4, el * pair, cw), BF),
            pltpu.VMEM((NK, 4 * b, cw), F32),
            pltpu.VMEM((NK, 2, 2, b, cw // 2), F32),
            pltpu.VMEM((NK, 2, b, cw // 2), F32),
            pltpu.VMEM((N1, 2, cw, ff), BF),
            pltpu.VMEM((N2, ff, cw), BF),
            dma((N1, 2)), dma((N2,)),
            dma((7,)), dma((7,)),
            dma((NK, 7)), dma((NK, 7)), dma((NK,)),
            dma((NK,)), dma((NK,)),
            dma((NK, 2, 2)), dma((NK, 2, 2)),
            dma((NK, 2)), dma((NK, 2)),
        ],
        compiler_params=pltpu.CompilerParams(
            collective_id=0, has_side_effects=True, vmem_limit_bytes=67043328),
        name='moe',
    )(u, h, tab, w1, w3, w2, ws1, ws3, ws2)


def solution(mesh):
    ey, ex = mesh.shape['ey'], mesh.shape['ex']
    ndev = ey * ex
    rows = P(('ey', 'ex'))
    rep = P()

    def local(x, kv_k, kv_v, lens, topk_idx, gates, ln1, ln2, wq, wo, ws1, ws3, ws2, w1, w3, w2):
        b = x.shape[0]
        n_exp = w1.shape[0] * ndev
        cap = max(4, (2 * b * topk_idx.shape[1] + n_exp - 1) // n_exp)
        h, u, tab = _attention(x, kv_k, kv_v, lens, topk_idx, gates, ln1, ln2, wq, wo, w1.shape[0], ndev, cap)
        return _moe(u, h, tab, w1, w3, w2, ws1, ws3, ws2, cap)

    return jax.shard_map(
        local, mesh=mesh,
        in_specs=(rows, rows, rows, rows, rows, rows, rep, rep, rep, rep, rep, rep, rep, rows, rows, rows),
        out_specs=rows, check_vma=False)
```

```python
import functools

import jax
import jax.numpy as jnp
from jax import lax
from jax.experimental import pallas as pl
from jax.experimental.pallas import tpu as pltpu
from jax.sharding import PartitionSpec as P

EPS = 1e-6
BF = jnp.bfloat16
F32 = jnp.float32
MESH = pl.DeviceIdType.MESH
NK = 4
N1 = 4
N2 = 6
GS = 16
NS = 4
SHORT = 64
PIECES = 3


def _rms(v, w):
    v = v.astype(F32)
    r = lax.rsqrt(jnp.mean(v * v, axis=-1, keepdims=True) + EPS)
    return (v * r * w.astype(F32)).astype(BF)


def _attn_kernel(dims, lens_ref, x_ref, kv_k, kv_v, topk_ref, gates_ref, ln1_ref, ln2_ref, wq, wo,
                 h_ref, u_ref, tab_ref, wqb, wob, kb, vb, qs, os, oall, sb, pb, sq, so, sk):
    b, d, l, dh, nq, el, cap = dims
    hd = nq * dh
    qc = hd // 4
    ng = b // GS
    np_ = GS // 2

    def cpq(n):
        return pltpu.make_async_copy(wq.at[:, pl.ds(n * qc, qc)], wqb.at[n], sq.at[n])

    def cpo(n):
        return pltpu.make_async_copy(wo.at[:, pl.ds(n * qc, qc)], wob.at[n], so.at[n])

    for n in range(4):
        cpq(n).start()

    def fetch(g):
        slot = g % NS
        for i in range(GS):
            def copy(n, i=i):
                for src, dst in ((kv_k, kb), (kv_v, vb)):
                    pltpu.make_async_copy(
                        src.at[g * GS + i, pl.ds(0, n), :],
                        dst.at[slot, i // 2, pl.ds(0, n), pl.ds((i % 2) * dh, dh)], sk.at[slot]).start()

            lax.cond(lens_ref[g * GS + i] > SHORT, lambda: copy(l), lambda: copy(SHORT))

    def fetched(g):
        slot = g % NS
        full = jnp.int32(0)
        for i in range(GS):
            full = full + (lens_ref[g * GS + i] > SHORT).astype(jnp.int32)

        def wait(n):
            blk = kb.at[slot, 0, pl.ds(0, n), :]
            pltpu.make_async_copy(blk, blk, sk.at[slot]).wait()
            return 0

        lax.fori_loop(0, full, lambda i, _: wait(l), 0)
        lax.fori_loop(full, GS, lambda i, _: wait(SHORT), 0)

    def clear(s, _):
        for p in range(np_):
            kb[s, p] = jnp.zeros((l, 2 * dh), BF)
            vb[s, p] = jnp.zeros((l, 2 * dh), BF)
        return 0
    lax.fori_loop(0, NS, clear, 0)
    for g in range(NS - 2):
        fetch(jnp.int32(g))
    for n in range(4):
        cpo(n).start()

    n_exp = tab_ref.shape[0] * el
    eidx = lax.broadcasted_iota(jnp.int32, (n_exp, b), 0)
    hit = eidx < 0
    gate = jnp.zeros((n_exp, b), F32)
    for j in range(topk_ref.shape[0]):
        m = topk_ref[j:j + 1, :] == eidx
        hit = hit | m
        gate = gate + jnp.where(m, gates_ref[j:j + 1, :], 0.0)
    chosen = jnp.where(hit, 1.0, 0.0)
    tri = jnp.where(lax.broadcasted_iota(jnp.int32, (b, b), 0) < lax.broadcasted_iota(jnp.int32, (b, b), 1), 1.0, 0.0)
    before = jnp.dot(chosen.astype(BF), tri.astype(BF), preferred_element_type=F32)
    off = (lax.axis_index('ex') * cap).astype(F32)
    slot_ = jnp.where(hit & (before < cap), before + off, -1.0)
    for e in range(tab_ref.shape[0]):
        tab_ref[e, 0] = slot_[e * el:(e + 1) * el]
        tab_ref[e, 1] = gate[e * el:(e + 1) * el]

    a = _rms(x_ref[...], ln1_ref[...].reshape(1, d))
    for n in range(4):
        cpq(n).wait()
        qn = jnp.dot(a, wqb[n], preferred_element_type=F32).astype(BF).astype(F32)
        for i in range(qc // dh):
            qs[:, n * (qc // dh) + i, :] = qn[:, i * dh:(i + 1) * dh]

    pos = lax.broadcasted_iota(jnp.int32, (nq, l), 1)
    zero = jnp.zeros((nq, dh), BF)

    def scores(g):
        slot = g % NS
        for p in range(np_):
            s0 = g * GS + 2 * p
            q0 = jnp.concatenate([qs[s0].astype(BF), zero], axis=1)
            q1 = jnp.concatenate([zero, qs[s0 + 1].astype(BF)], axis=1)
            lhs = jnp.concatenate([q0, q1], axis=0)
            sb[p] = lax.dot_general(lhs, kb[slot, p], (((1,), (1,)), ((), ())), preferred_element_type=F32)

    def softmax(g):
        for p in range(np_):
            s0 = g * GS + 2 * p
            valid = jnp.concatenate([pos < lens_ref[s0], pos < lens_ref[s0 + 1]], axis=0)
            s = jnp.where(valid, sb[p] * dh ** -0.5, -jnp.inf)
            e = jnp.exp(s - jnp.max(s, axis=-1, keepdims=True))
            pb[p] = (e * (1.0 / jnp.sum(e, axis=-1, keepdims=True))).astype(BF)

    def values(g):
        slot = g % NS
        for p in range(np_):
            s0 = g * GS + 2 * p
            o = jnp.dot(pb[p], vb[slot, p], preferred_element_type=F32).astype(BF).astype(F32)
            os[s0] = o[0:nq, 0:dh]
            os[s0 + 1] = o[nq:2 * nq, dh:2 * dh]

    fetched(jnp.int32(0))
    scores(jnp.int32(0))
    fetch(jnp.int32(NS - 2))
    fetched(jnp.int32(1))
    softmax(jnp.int32(0))
    scores(jnp.int32(1))
    fetch(jnp.int32(NS - 1))

    def step(g, _):
        fetched(g)
        values(g - 2)
        softmax(g - 1)
        scores(g)

        @pl.when(g - 2 + NS < ng)
        def _():
            fetch(g - 2 + NS)
        return 0

    lax.fori_loop(2, ng, step, 0)
    values(jnp.int32(ng - 2))
    softmax(jnp.int32(ng - 1))
    values(jnp.int32(ng - 1))
    for i in range(nq):
        oall[:, i * dh:(i + 1) * dh] = os[:, i, :].astype(BF)
    for n in range(4):
        cpo(n).wait()
        cs = slice(n * qc, (n + 1) * qc)
        h_ref[:, cs] = (x_ref[:, cs].astype(F32)
                        + jnp.dot(oall[...], wob[n], preferred_element_type=F32)).astype(BF)
    u_ref[...] = _rms(h_ref[...], ln2_ref[...].reshape(1, d))


def _attention(x, kv_k, kv_v, lens, topk, gates, ln1, ln2, wq, wo, el, ndev, cap):
    b, d = x.shape
    _, l, kvh, dh = kv_k.shape
    hd = wq.shape[1]
    nq = hd // dh
    vm = pl.BlockSpec(memory_space=pltpu.VMEM)
    hb = pl.BlockSpec(memory_space=pltpu.HBM)
    sm = pl.BlockSpec(memory_space=pltpu.SMEM)
    dma = pltpu.SemaphoreType.DMA
    return pl.pallas_call(
        functools.partial(_attn_kernel, (b, d, l, dh, nq, el, cap)),
        out_shape=(jax.ShapeDtypeStruct((b, d), BF), jax.ShapeDtypeStruct((b, d), BF),
                   jax.ShapeDtypeStruct((ndev, 2, el, b), F32)),
        in_specs=[sm, vm, hb, hb, vm, vm, vm, vm, hb, hb],
        out_specs=(vm, vm, vm),
        scratch_shapes=[
            pltpu.VMEM((4, d, hd // 4), BF),
            pltpu.VMEM((4, hd, d // 4), BF),
            pltpu.VMEM((NS, GS // 2, l, 2 * dh), BF),
            pltpu.VMEM((NS, GS // 2, l, 2 * dh), BF),
            pltpu.VMEM((b, nq, dh), F32),
            pltpu.VMEM((b, nq, dh), F32),
            pltpu.VMEM((b, hd), BF),
            pltpu.VMEM((GS // 2, 2 * nq, l), F32),
            pltpu.VMEM((GS // 2, 2 * nq, l), BF),
            dma((4,)), dma((4,)), dma((NS,)),
        ],
        compiler_params=pltpu.CompilerParams(vmem_limit_bytes=56 * 1024 * 1024),
        name='attn',
    )(lens, x, kv_k.reshape(b, l, dh), kv_v.reshape(b, l, dh), topk.T, gates.T,
      ln1, ln2, wq, wo)


def _moe_kernel(dims, u_ref, h_ref, tab_ref, w1, w3, w2, ws1, ws3, ws2, y_ref,
                uall, tabs, sel, wgt, xin, acc, z, zs, sh, outb, d2d, rx1, rx2, r13, r2,
                s13, sw2, tsend, trecv, usend, urecv, uloc, dsend, drecv, psend, precv, qsend, qrecv):
    b, d, ff, el, cap = dims
    cw = d // NK
    pair = 2 * cap
    rows = 4 * pair
    ey = lax.axis_index('ey')
    ex = lax.axis_index('ex')
    me = ey * 2 + ex
    ox = 1 - ex
    cx, cy = ey % 2, ey // 2
    xn = cy * 2 + (1 - cx)
    yn = (1 - cy) * 2 + cx
    dg = (1 - cy) * 2 + (1 - cx)
    partner, xdev, ydev = (ey, ox), (xn, ex), (yn, ex)

    n13 = NK + NK * el
    n2 = NK * (el + 1)

    def cp13(src, slot, i):
        return pltpu.make_async_copy(src, r13.at[slot, i], s13.at[slot, i])

    def start13(s):
        slot = s % N1

        @pl.when(s < NK)
        def _():
            ks = pl.ds(pl.multiple_of(s * cw, cw), cw)
            cp13(ws1.at[ks, :], slot, 0).start()
            cp13(ws3.at[ks, :], slot, 1).start()

        @pl.when(s >= NK)
        def _():
            t = s - NK
            e = t % el
            ks = pl.ds(pl.multiple_of((t // el) * cw, cw), cw)
            cp13(w1.at[e, ks, :], slot, 0).start()
            cp13(w3.at[e, ks, :], slot, 1).start()

    def wait13(s):
        slot = s % N1
        for i in range(2):
            cp13(w1.at[0, pl.ds(0, cw), :], slot, i).wait()

    def start2(j):
        slot = j % N2
        c = j // (el + 1)
        i = j % (el + 1)
        cs = pl.ds(pl.multiple_of(c * cw, cw), cw)

        @pl.when(i < el)
        def _():
            pltpu.make_async_copy(w2.at[i, :, cs], r2.at[slot], sw2.at[slot]).start()

        @pl.when(i == el)
        def _():
            pltpu.make_async_copy(ws2.at[:, cs], r2.at[slot], sw2.at[slot]).start()

    def wait2(j):
        slot = j % N2
        pltpu.make_async_copy(w2.at[0, :, pl.ds(0, cw)], r2.at[slot], sw2.at[slot]).wait()

    for s in range(N1):
        start13(jnp.int32(s))
    for j in range(N2):
        start2(jnp.int32(j))

    barrier = pltpu.get_barrier_semaphore()
    for o in range(1, 8):
        peer = (me + o) % 8
        pl.semaphore_signal(barrier, inc=1, device_id=(peer // 2, peer % 2), device_id_type=MESH)
    pl.semaphore_wait(barrier, 7)

    def ublk(k, chip, e):
        return uall.at[k, chip, pl.ds(pl.multiple_of(e * b, b), b), :]

    def ucopy(k, i, src, chip, e, role, dev):
        return pltpu.make_async_remote_copy(
            src_ref=src, dst_ref=ublk(k, chip, e), send_sem=usend.at[k, i], recv_sem=urecv.at[k, role],
            device_id=dev, device_id_type=MESH)

    def uown(k):
        return u_ref.at[:, pl.ds(k * cw, cw)]

    def direct(k):
        cps = [ucopy(k, 1, uown(k), ey, ex, 1, xdev), ucopy(k, 2, uown(k), ey, ex, 2, ydev),
               ucopy(k, 0, uown(k), ey, ex, 0, partner)]
        for cp in cps:
            cp.start()
        pltpu.make_async_copy(uown(k), ublk(k, ey, ex), uloc.at[k]).start()

    def urcv(k, role, chip, e):
        return ucopy(k, 0, uown(k), chip, e, role, partner)

    def forward(k):
        urcv(k, 1, xn, ex).wait_recv()
        if k % 2 == 0:
            ucopy(k, 3, ublk(k, xn, ex), xn, ex, 3, ydev).start()
        ucopy(k, 4, ublk(k, xn, ex), xn, ex, 4, partner).start()
        urcv(k, 2, yn, ex).wait_recv()
        if k % 2 == 1:
            ucopy(k, 3, ublk(k, yn, ex), yn, ex, 3, xdev).start()
        ucopy(k, 5, ublk(k, yn, ex), yn, ex, 5, partner).start()

    def forward_diag(k):
        urcv(k, 3, dg, ex).wait_recv()
        ucopy(k, 6, ublk(k, dg, ex), dg, ex, 6, partner).start()

    def arrived(k):
        pltpu.make_async_copy(uown(k), ublk(k, ey, ex), uloc.at[k]).wait()
        urcv(k, 0, ey, ox).wait_recv()
        urcv(k, 4, xn, ox).wait_recv()
        urcv(k, 5, yn, ox).wait_recv()
        urcv(k, 6, dg, ox).wait_recv()

    direct(0)

    def tcopy(o, peer):
        return pltpu.make_async_remote_copy(
            src_ref=tab_ref.at[peer], dst_ref=tabs.at[me], send_sem=tsend.at[o - 1], recv_sem=trecv.at[o - 1],
            device_id=(peer // 2, peer % 2), device_id_type=MESH)

    for o in range(1, 8):
        tcopy(o, (me + o) % 8).start()
    tabs[me] = tab_ref[me]
    direct(1)

    def silu_mul(g, v):
        return (g * (1.0 / (1.0 + jnp.exp(-g))) * v).astype(BF)

    nts = [(n, min(512, ff - n)) for n in range(0, ff, 512)]

    for s in range(NK):
        wait13(s)
        for n, nw in nts:
            for i in range(2):
                p = jnp.dot(u_ref[:, s * cw:(s + 1) * cw], r13[s % N1, i, :, n:n + nw], preferred_element_type=F32)
                if s > 0:
                    p = acc[i, 0:b, n:n + nw] + p
                acc[i, 0:b, n:n + nw] = p
        start13(jnp.int32(s + N1))
    for n, nw in nts:
        zs[:, n:n + nw] = silu_mul(acc[0, 0:b, n:n + nw], acc[1, 0:b, n:n + nw])

    forward(0)
    direct(2)

    for o in range(1, 8):
        src = (me + 8 - o) % 8
        pltpu.make_async_remote_copy(
            src_ref=tab_ref.at[src], dst_ref=tabs.at[src], send_sem=tsend.at[o - 1], recv_sem=trecv.at[o - 1],
            device_id=(src // 2, src % 2), device_id_type=MESH).wait_recv()
    iota = lax.broadcasted_iota(jnp.int32, (pair, 2 * b), 0).astype(F32)

    def build(c, _):
        t = jnp.concatenate([tabs[2 * c, 0], tabs[2 * c + 1, 0]], axis=1)
        g = jnp.concatenate([tabs[2 * c, 1], tabs[2 * c + 1, 1]], axis=1)
        one = []
        gat = []
        for e in range(el):
            m = iota == t[e:e + 1, :]
            one.append(jnp.where(m, 1.0, 0.0))
            gat.append(jnp.where(m, g[e:e + 1, :], 0.0))
        sel[c] = jnp.concatenate(one, axis=0).astype(BF)
        gt = jnp.concatenate(gat, axis=0).T
        for i in range(PIECES):
            piece = gt.astype(BF)
            wgt[i, c] = piece
            gt = gt - piece.astype(F32)
        return 0

    lax.fori_loop(0, 4, build, 0)

    forward(1)
    direct(3)
    forward_diag(0)
    events = {(0, 2): lambda: forward(2), (0, 4): lambda: forward_diag(1), (0, 6): lambda: forward(3),
              (1, 2): lambda: forward_diag(2), (1, 4): lambda: forward_diag(3)}

    def down_one(j, e):
        r = jnp.dot(z[e], r2[j % N2], preferred_element_type=F32).astype(BF)
        for q in range(4):
            outb[q, pl.ds(pl.multiple_of(e * pair, pair), pair), :] = r[q * pair:(q + 1) * pair, :]

    for k in range(NK):
        arrived(k)

        def pick(c, _, k=k):
            r = jnp.dot(sel[c], uall[k, c], preferred_element_type=F32).astype(BF)
            for e in range(el):
                xin[e, pl.ds(pl.multiple_of(c * pair, pair), pair), :] = r[e * pair:(e + 1) * pair, :]
            return 0

        lax.fori_loop(0, 4, pick, 0)

        def zstep(e, _, k=k):
            for (ke, at), event in events.items():
                if ke == k:
                    pl.when(e == at)(event)
            s = NK + k * el + e
            wait13(s)
            slot = s % N1
            er = pl.ds(pl.multiple_of(e * rows, rows), rows)
            for n, nw in nts:
                ps = []
                for i in range(2):
                    p = jnp.dot(xin[e], r13[slot, i, :, n:n + nw], preferred_element_type=F32)
                    if k > 0:
                        p = acc[i, er, n:n + nw] + p
                    ps.append(p)
                if k < NK - 1:
                    acc[0, er, n:n + nw] = ps[0]
                    acc[1, er, n:n + nw] = ps[1]
                else:
                    z[e, :, n:n + nw] = silu_mul(ps[0], ps[1])
            nxt = s + N1

            @pl.when(nxt < n13)
            def _():
                start13(nxt)

            if k == NK - 1:
                wait2(e)
                down_one(e, e)
                start2(e + N2)
            return 0

        lax.fori_loop(0, el, zstep, 0)

    hw = cw // 2

    def part(c, e, chip, j=None):
        cols = pl.ds((c % 2) * cw, cw) if j is None else pl.ds((c % 2) * cw + j * hw, hw)
        return acc.at[c // 2, pl.ds(pl.multiple_of((e * 4 + chip) * b, b), b), cols]

    order = ((xn, xdev, yn, ydev), (yn, ydev, xn, xdev))

    def dcopy(c, t):
        rs = pl.ds(pl.multiple_of((ox * 4 + 2 * t) * b, b), 2 * b)
        return pltpu.make_async_remote_copy(
            src_ref=acc.at[c // 2, rs, pl.ds((c % 2) * cw, cw)],
            dst_ref=d2d.at[c, pl.ds(pl.multiple_of(2 * t * b, b), 2 * b)],
            send_sem=dsend.at[c, t], recv_sem=drecv.at[c, t], device_id=partner, device_id_type=MESH)

    def pcopy(c, j, i):
        first, dev, _, _ = order[j]
        return pltpu.make_async_remote_copy(
            src_ref=part(c, ex, first if i == 0 else dg, j), dst_ref=rx1.at[c, j, i], send_sem=psend.at[c, j, i],
            recv_sem=precv.at[c, j, i], device_id=dev, device_id_type=MESH)

    def qcopy(c, j):
        _, _, second, dev = order[j]
        return pltpu.make_async_remote_copy(
            src_ref=part(c, ex, second, j), dst_ref=rx2.at[c, j], send_sem=qsend.at[c, j], recv_sem=qrecv.at[c, j],
            device_id=dev, device_id_type=MESH)

    def step_a(c, events):
        def down(t, _):
            for at, event in events:
                pl.when(t == at)(event)
            for i in range(2):
                wait2(c * (el + 1) + 2 * t + i)
            for i in range(2):
                down_one(c * (el + 1) + 2 * t + i, 2 * t + i)
            for i in range(2):
                j = c * (el + 1) + 2 * t + i

                @pl.when(j + N2 < n2)
                def _(j=j):
                    start2(j + N2)
            return 0

        if c > 0:
            lax.fori_loop(0, el // 2, down, 0)

        def comb(t, _):
            for i in range(2):
                q = 2 * t + i
                p = jnp.dot(wgt[0, q], outb[q], preferred_element_type=F32)
                for n in range(1, PIECES):
                    p = p + jnp.dot(wgt[n, q], outb[q], preferred_element_type=F32)
                part(c, 0, q)[...] = p[0:b]
                part(c, 1, q)[...] = p[b:2 * b]
            dcopy(c, t).start()
            return 0

        lax.fori_loop(0, 2, comb, 0)
        j = c * (el + 1) + el
        wait2(jnp.int32(j))
        sh[:, c * cw:(c + 1) * cw] = jnp.dot(zs[...], r2[j % N2], preferred_element_type=F32).astype(BF)
        if j + N2 < n2:
            start2(jnp.int32(j + N2))

    def step_b(c):
        dcopy(c, 0).wait_recv()
        dcopy(c, 1).wait_recv()

        def add(q, _):
            part(c, ex, q)[...] = part(c, ex, q)[...] + d2d[c, pl.ds(pl.multiple_of(q * b, b), b), :]
            return 0

        lax.fori_loop(0, 4, add, 0)
        for i in (1, 0):
            for j in range(2):
                pcopy(c, j, i).start()

    def step_c(c):
        for j in range(2):
            pcopy(c, j, 1).wait_recv()
            second = order[j][2]
            part(c, ex, second, j)[...] = part(c, ex, second, j)[...] + rx1[c, j, 1]
            qcopy(c, j).start()

    def step_d(c):
        for j in range(2):
            pcopy(c, j, 0).wait_recv()
            qcopy(c, j).wait_recv()
            cs = slice(c * cw + j * hw, c * cw + (j + 1) * hw)
            t = part(c, ex, ey, j)[...] + rx1[c, j, 0] + rx2[c, j]
            y_ref[:, cs] = (h_ref[:, cs].astype(F32) + sh[:, cs].astype(F32) + t).astype(BF)

    step_a(0, ())
    step_a(1, ((1, lambda: step_b(0)),))
    step_a(2, ((0, lambda: step_c(0)), (1, lambda: step_b(1))))
    step_a(3, ((0, lambda: step_c(1)), (1, lambda: step_b(2))))
    step_b(3)
    step_c(2)
    step_d(0)
    step_d(1)
    step_c(3)
    step_d(2)
    step_d(3)

    for o in range(1, 8):
        tcopy(o, (me + o) % 8).wait_send()
    for k in range(NK):
        for i in range(7):
            ucopy(k, i, uown(k), ey, ex, 0, partner).wait_send()
    for c in range(NK):
        dcopy(c, 0).wait_send()
        dcopy(c, 1).wait_send()
        for j in range(2):
            pcopy(c, j, 0).wait_send()
            pcopy(c, j, 1).wait_send()
            qcopy(c, j).wait_send()


def _moe(u, h, tab, w1, w3, w2, ws1, ws3, ws2, cap):
    b, d = u.shape
    el, _, ff = w1.shape
    ndev, _, _, _ = tab.shape
    cw = d // NK
    pair = 2 * cap
    rows = 4 * pair
    vm = pl.BlockSpec(memory_space=pltpu.VMEM)
    hb = pl.BlockSpec(memory_space=pltpu.HBM)
    dma = pltpu.SemaphoreType.DMA
    return pl.pallas_call(
        functools.partial(_moe_kernel, (b, d, ff, el, cap)),
        out_shape=jax.ShapeDtypeStruct((b, d), BF),
        in_specs=[vm, vm, vm, hb, hb, hb, hb, hb, hb],
        out_specs=vm,
        scratch_shapes=[
            pltpu.VMEM((NK, 4, 2 * b, cw), BF),
            pltpu.VMEM((ndev, 2, el, b), F32),
            pltpu.VMEM((4, el * pair, 2 * b), BF),
            pltpu.VMEM((PIECES, 4, 2 * b, el * pair), BF),
            pltpu.VMEM((el, rows, cw), BF),
            pltpu.VMEM((2, el * rows, ff), F32),
            pltpu.VMEM((el, rows, ff), BF),
            pltpu.VMEM((b, ff), BF),
            pltpu.VMEM((b, d), BF),
            pltpu.VMEM((4, el * pair, cw), BF),
            pltpu.VMEM((NK, 4 * b, cw), F32),
            pltpu.VMEM((NK, 2, 2, b, cw // 2), F32),
            pltpu.VMEM((NK, 2, b, cw // 2), F32),
            pltpu.VMEM((N1, 2, cw, ff), BF),
            pltpu.VMEM((N2, ff, cw), BF),
            dma((N1, 2)), dma((N2,)),
            dma((7,)), dma((7,)),
            dma((NK, 7)), dma((NK, 7)), dma((NK,)),
            dma((NK, 2)), dma((NK, 2)),
            dma((NK, 2, 2)), dma((NK, 2, 2)),
            dma((NK, 2)), dma((NK, 2)),
        ],
        compiler_params=pltpu.CompilerParams(
            collective_id=0, has_side_effects=True, vmem_limit_bytes=67043328),
        name='moe',
    )(u, h, tab, w1, w3, w2, ws1, ws3, ws2)


def solution(mesh):
    ey, ex = mesh.shape['ey'], mesh.shape['ex']
    ndev = ey * ex
    rows = P(('ey', 'ex'))
    rep = P()

    def local(x, kv_k, kv_v, lens, topk_idx, gates, ln1, ln2, wq, wo, ws1, ws3, ws2, w1, w3, w2):
        b = x.shape[0]
        n_exp = w1.shape[0] * ndev
        cap = max(4, (2 * b * topk_idx.shape[1] + n_exp - 1) // n_exp)
        h, u, tab = _attention(x, kv_k, kv_v, lens, topk_idx, gates, ln1, ln2, wq, wo, w1.shape[0], ndev, cap)
        return _moe(u, h, tab, w1, w3, w2, ws1, ws3, ws2, cap)

    return jax.shard_map(
        local, mesh=mesh,
        in_specs=(rows, rows, rows, rows, rows, rows, rep, rep, rep, rep, rep, rep, rep, rows, rows, rows),
        out_specs=rows, check_vma=False)
```
